128 devices in a mesh: dp: 4 (over x_lo, core), tp: 32 (over y, x_hi, z).
Axes of the slice: x: 4 (x_hi: 2, x_lo: 2; x = x_hi * 2 + x_lo), y: 4, z: 4, core: 2. Of those that a mesh axis runs over, the one named last changes fastest.
Arguments:
- layer_inputs: bfloat16 [2, 1536, 4608], P(None, 'dp'), may hold values from -120 to 120
- out_grad: bfloat16 [1536, 4608], P('dp'), may hold values from -6 to 6
- gain: float32 [2, 4608], replicated, may hold values from 0.5 to 1.5
- w_query: bfloat16 [2, 4608, 4096], P(None, None, 'tp'), may hold values from -0.09375 to 0.09375
- w_key: bfloat16 [2, 4608, 2048], P(None, None, 'tp'), may hold values from -0.09375 to 0.09375
- w_value: bfloat16 [2, 4608, 2048], P(None, None, 'tp'), may hold values from -0.09375 to 0.09375
- w_out: bfloat16 [2, 4096, 4608], P(None, 'tp'), may hold values from -0.09375 to 0.09375
- doc_lengths: int32 [4, 4], P('dp'), may hold values from 1 to 192, 384 in all within a row
- window_reach: int32 [2], replicated, may hold values from 48 to 384, as said below
Outputs:
- input_grad: bfloat16 [1536, 4608], P('dp')
- grad_w_query: float32 [2, 4608, 4096], P(None, 'dp', 'tp')
- grad_w_key: float32 [2, 4608, 2048], P(None, 'dp', 'tp')
- grad_w_value: float32 [2, 4608, 2048], P(None, 'dp', 'tp')
- grad_w_out: float32 [2, 4096, 4608], P(None, 'tp', 'dp')
- grad_gain: float32 [2, 4608], replicated
The draws below stay inside these ranges and needn't reach their ends.
Inputs may be any that keep to these rules, and one draw needn't show every extreme that they name: `doc_lengths`: the 4 lengths of a row fill its sequence's 384 positions in order; in every row the longest document has exactly 192 positions. `window_reach`: exactly one sublayer has reach 384 (it sees all earlier positions of its document); the other's reach is at most 192.
All inputs are finite; a program needn't handle non-finite values.
Results may differ from the reference program's by a relative error of at most 0.025.
Values may be sent and summed in bfloat16 or wider, within the bound.
A program may use at most 128 MiB of HBM per device.

```python
import math
import jax
import jax.numpy as jnp
import numpy as np
from jax import lax

D = 4608
HEADS = 32
KV_HEADS = 16
HD = 128
SEQ_LEN = 384
LAYERS = 2
DOCS = 4
SEQUENCES = 4
TOKENS = 1536
N_DP = 4


def draw_layer_inputs(key, part):
    subkeys = jax.random.split(jax.random.fold_in(key, 11), 3)
    full_shape = (LAYERS, TOKENS, D)
    row_scale = jnp.exp(jax.random.uniform(subkeys[0], (LAYERS, TOKENS, 1), jnp.float32, 0.0, math.log(10.0)))
    col_scale = jnp.exp(jax.random.uniform(subkeys[1], (LAYERS, 1, D), jnp.float32, math.log(0.3), math.log(3.0)))
    entries = jnp.clip(jax.random.normal(subkeys[2], full_shape, jnp.float32), -4.0, 4.0)
    return (entries * row_scale * col_scale).astype(jnp.bfloat16)


def draw_window_reach(key, part):
    subkeys = jax.random.split(jax.random.fold_in(key, 23), 2)
    span = jax.random.randint(subkeys[0], (), SEQ_LEN // 8, SEQ_LEN // 2 + 1, jnp.int32)
    which = jax.random.randint(subkeys[1], (), 0, LAYERS, jnp.int32)
    layer_index = jnp.arange(LAYERS, dtype=jnp.int32)
    return jnp.where(layer_index == which, jnp.int32(SEQ_LEN), span).astype(jnp.int32)


def block_scale(stream_key, dims, pieces, smallest, top_value):
    def one(dim, blocks):
        steps = jax.random.uniform(jax.random.fold_in(jax.random.fold_in(stream_key, 6), dim), (blocks,), jnp.float32, smallest / len(pieces), top_value / len(pieces))
        return jnp.repeat(jnp.exp(steps), dims[dim] // blocks).reshape((-1,) + (1,) * (len(dims) - dim - 1))

    level = one(*pieces[0])
    for cut in pieces[1:]:
        level = level * one(*cut)
    return level


def profile(amount, total, bound, skew):
    portions = [(1 << 20) // math.isqrt(standing ** skew) + 1 for standing in range(2, amount + 1)]
    surplus, holding = total - bound - (amount - 1), [1] * (amount - 1)
    while surplus > 0:
        candidates = [i for i in range(amount - 1) if holding[i] < bound]
        pool, budget = sum([portions[i] for i in candidates]), surplus
        for i in candidates:
            more = min(bound - holding[i], max(1, budget * portions[i] // pool), surplus)
            holding[i] = holding[i] + more
            surplus = surplus - more
    return np.array([bound] + holding)


def ragged_sizes(stream_key, number_of, total, bound, lean):
    if number_of == 2:
        one = jax.random.randint(stream_key, (), max(1, total - bound), min(bound, total - 1) + 1)
        return jnp.stack([one, total - one])
    sizes = jnp.asarray(profile(number_of, total, bound, lean), jnp.int32)
    twos = (number_of - 1) // 2
    giver, sink = sizes[1:1 + 2 * twos:2], sizes[2:2 + 2 * twos:2]
    slack = jnp.minimum(giver - 1, bound - sink)
    moved = jax.random.randint(jax.random.fold_in(stream_key, 1), (twos,), 0, 1 << 20) % (slack + 1)
    sizes = sizes.at[1:1 + 2 * twos:2].set(giver - moved).at[2:2 + 2 * twos:2].set(sink + moved)
    return sizes[jax.random.permutation(jax.random.fold_in(stream_key, 2), number_of)]


def scatter_about(key, dims, scale, most, cuts=(), kind=jnp.bfloat16):
    values = scale * jax.random.normal(key, dims, jnp.float32)
    if cuts:
        values = values * block_scale(key, dims, cuts, -0.22, 0.18)
    return jnp.clip(values, -most, most).astype(kind)


def setup_inputs(seed: int = 0) -> dict:
    streams_of = jax.random.split(jax.random.key(seed), 10)
    layer_inputs = draw_layer_inputs(jax.random.fold_in(streams_of[9], 71), 0)
    out_grad = scatter_about(streams_of[1], (TOKENS, D), 1.0, 6.0, ((0, 4),))
    gain = jnp.clip(1.0 + 0.1 * jax.random.normal(streams_of[2], (LAYERS, D), jnp.float32), 0.5, 1.5)
    w_query = scatter_about(streams_of[3], (LAYERS, D, HEADS * HD), D ** -0.5, 0.09375, ((2, 32),))
    w_key = scatter_about(streams_of[4], (LAYERS, D, KV_HEADS * HD), D ** -0.5, 0.09375, ((2, 32),))
    w_value = scatter_about(streams_of[5], (LAYERS, D, KV_HEADS * HD), D ** -0.5, 0.09375, ((2, 32),))
    w_out = scatter_about(streams_of[6], (LAYERS, HEADS * HD, D), (HEADS * HD) ** -0.5, 0.09375, ((1, 32),))
    doc_lengths = jax.vmap(lambda own: ragged_sizes(own, DOCS, SEQ_LEN, SEQ_LEN // 2, 2))(jax.random.split(streams_of[7], SEQUENCES)).reshape((SEQUENCES, DOCS)).astype(jnp.int32)
    window_reach = draw_window_reach(jax.random.fold_in(streams_of[9], 71), 0)
    return {"layer_inputs": layer_inputs, "out_grad": out_grad, "gain": gain, "w_query": w_query, "w_key": w_key, "w_value": w_value, "w_out": w_out, "doc_lengths": doc_lengths, "window_reach": window_reach}


softcap = 50.0
epsilon = 1e-06

def rope_tables(length, head_width):
    half_width = head_width // 2
    frequencies = jnp.exp(-jnp.arange(half_width).astype(jnp.float32) * (2.0 * math.log(10000.0) / head_width))
    angles = jnp.arange(length).astype(jnp.float32)[:, None] * frequencies[None, :]
    return (jnp.cos(angles)[:, None, :], jnp.sin(angles)[:, None, :])

def rotate(values, cosine, sine_table):
    half_width = values.shape[-1] // 2
    first_half = values[..., :half_width]
    second_half = values[..., half_width:]
    return jnp.concatenate([first_half * cosine - second_half * sine_table, second_half * cosine + first_half * sine_table], axis=-1)

def unrotate(values, cosine, sine_table):
    half_width = values.shape[-1] // 2
    first_half = values[..., :half_width]
    second_half = values[..., half_width:]
    return jnp.concatenate([first_half * cosine + second_half * sine_table, second_half * cosine - first_half * sine_table], axis=-1)

def allowed_pairs(lengths_row, reach, length):
    doc_ends = jnp.cumsum(lengths_row.astype(jnp.int32))
    places = jnp.arange(length, dtype=jnp.int32)
    document = lax.optimization_barrier(jnp.sum((places[:, None] >= doc_ends[None, :]).astype(jnp.int32), axis=1))
    same_doc = document[:, None] == document[None, :]
    causal = places[None, :] <= places[:, None]
    in_window = places[:, None] - places[None, :] < reach.astype(jnp.int32)
    return same_doc & causal & in_window

def layer_backward(inputs, upstream, gain_row, query_weight, key_weight, value_weight, out_weight, lengths_row, reach):
    length = inputs.shape[0]
    cosine, sine_table = rope_tables(length, HD)
    score_scale = (D // HEADS) ** (-0.5)
    allowed = allowed_pairs(lengths_row, reach, length)
    matrix_rows = inputs.astype(jnp.float32)
    reciprocal = lax.rsqrt(lax.optimization_barrier(jnp.mean(matrix_rows * matrix_rows, axis=-1, keepdims=True)) + epsilon)
    unit_rows = matrix_rows * reciprocal
    normed = (unit_rows * gain_row).astype(jnp.bfloat16)
    queries = rotate(jnp.dot(normed, query_weight, preferred_element_type=jnp.float32).reshape(length, HEADS, HD), cosine, sine_table).astype(jnp.bfloat16)
    keys_rope = rotate(jnp.dot(normed, key_weight, preferred_element_type=jnp.float32).reshape(length, KV_HEADS, HD), cosine, sine_table).astype(jnp.bfloat16)
    values_cast = jnp.dot(normed, value_weight, preferred_element_type=jnp.float32).reshape(length, KV_HEADS, HD).astype(jnp.bfloat16)
    keys_shared = jnp.repeat(keys_rope, 2, axis=1).astype(jnp.float32)
    values_shared = jnp.repeat(values_cast, 2, axis=1).astype(jnp.float32)
    queries_float = queries.astype(jnp.float32)
    scores = jnp.einsum('thd,shd->hts', queries_float, keys_shared) * score_scale
    squashed = jnp.tanh(scores / softcap)
    raised = jnp.where(allowed[None], jnp.exp(softcap * squashed), 0.0)
    probability = raised / lax.optimization_barrier(jnp.sum(raised, axis=-1, keepdims=True))
    rounded_prob = probability.astype(jnp.bfloat16)
    attended = jnp.einsum('hts,shd->thd', rounded_prob.astype(jnp.float32), values_shared).astype(jnp.bfloat16)
    attended_flat = attended.reshape(length, HEADS * HD)
    grad_attended = jnp.dot(upstream, out_weight.T, preferred_element_type=jnp.float32).astype(jnp.bfloat16)
    part_w_out = jnp.dot(attended_flat.T, upstream, preferred_element_type=jnp.float32)
    grad_heads = grad_attended.reshape(length, HEADS, HD).astype(jnp.float32)
    row_delta = lax.optimization_barrier(jnp.sum(grad_heads * attended.astype(jnp.float32), axis=-1)).T
    grad_probs = jnp.einsum('thd,shd->hts', grad_heads, values_shared)
    grad_scores = (probability * (grad_probs - row_delta[:, :, None]) * (1.0 - squashed * squashed) * score_scale).astype(jnp.bfloat16)
    score_grad_float = grad_scores.astype(jnp.float32)
    grad_queries = unrotate(jnp.einsum('hts,shd->thd', score_grad_float, keys_shared), cosine, sine_table).astype(jnp.bfloat16).reshape(length, HEADS * HD)
    key_each = unrotate(jnp.einsum('hts,thd->shd', score_grad_float, queries_float), cosine, sine_table).astype(jnp.bfloat16)
    value_each = jnp.einsum('hts,thd->shd', rounded_prob.astype(jnp.float32), grad_heads).astype(jnp.bfloat16)
    part_w_query = jnp.dot(normed.T, grad_queries, preferred_element_type=jnp.float32)
    grad_normed = jnp.dot(grad_queries, query_weight.T, preferred_element_type=jnp.float32)
    part_w_key = jnp.zeros(key_weight.shape, jnp.float32)
    part_w_value = jnp.zeros(value_weight.shape, jnp.float32)
    for parity in range(2):
        key_part = key_each[:, parity::2, :].reshape(length, KV_HEADS * HD)
        value_part = value_each[:, parity::2, :].reshape(length, KV_HEADS * HD)
        part_w_key = part_w_key + jnp.dot(normed.T, key_part, preferred_element_type=jnp.float32)
        part_w_value = part_w_value + jnp.dot(normed.T, value_part, preferred_element_type=jnp.float32)
        grad_normed = grad_normed + jnp.dot(key_part, key_weight.T, preferred_element_type=jnp.float32)
        grad_normed = grad_normed + jnp.dot(value_part, value_weight.T, preferred_element_type=jnp.float32)
    scaled_grad = grad_normed * gain_row
    branch = reciprocal * (scaled_grad - unit_rows * lax.optimization_barrier(jnp.mean(scaled_grad * unit_rows, axis=-1, keepdims=True)))
    layer_grad = (upstream.astype(jnp.float32) + branch).astype(jnp.bfloat16)
    gain_part = lax.optimization_barrier(jnp.sum(grad_normed * unit_rows, axis=0))
    return (layer_grad, part_w_query, part_w_key, part_w_value, part_w_out, gain_part)

def reference(layer_inputs, out_grad, gain, w_query, w_key, w_value, w_out, doc_lengths, window_reach):
    totals = [[None, None, None, None, None] for layer_number in range(LAYERS)]
    input_rows = []
    for sequence in range(N_DP):
        first_row = sequence * SEQ_LEN
        upstream = out_grad[first_row:first_row + SEQ_LEN]
        for layer_number in reversed(range(LAYERS)):
            results = layer_backward(layer_inputs[layer_number, first_row:first_row + SEQ_LEN], upstream, gain[layer_number], w_query[layer_number], w_key[layer_number], w_value[layer_number], w_out[layer_number], doc_lengths[sequence], window_reach[layer_number])
            upstream = results[0]
            for member in range(4):
                rounded = lax.optimization_barrier(results[member + 1].astype(jnp.bfloat16)).astype(jnp.float32)
                if totals[layer_number][member] is None:
                    totals[layer_number][member] = rounded
                else:
                    totals[layer_number][member] = totals[layer_number][member] + rounded
            if totals[layer_number][4] is None:
                totals[layer_number][4] = results[5]
            else:
                totals[layer_number][4] = totals[layer_number][4] + results[5]
        input_rows.append(upstream)
    input_grad = jnp.concatenate(input_rows, axis=0)
    stacks = [jnp.stack([totals[layer_number][member] for layer_number in range(LAYERS)]) / N_DP for member in range(5)]
    return (input_grad, stacks[0], stacks[1], stacks[2], stacks[3], stacks[4])
```

```python
import functools
import math

import jax
import jax.numpy as jnp
import numpy as np
from jax import lax
from jax.experimental import pallas as pl
from jax.experimental.pallas import tpu as pltpu
from jax.sharding import Mesh
from jax.sharding import PartitionSpec as P

D = 4608
HEADS = 32
HD = 128
SEQ = 384
LAYERS = 2
CB = D // 4
RB = 48
CA = 640
XL, CORE, Y, XH, Z = ("dp_0", "dp_1", "tp_0", "tp_1", "tp_2")
TP = (Y, XH, Z)
DP = (XL, CORE)
MESH = pl.DeviceIdType.MESH
VMEM = pltpu.VMEM
F32 = jnp.float32
BF16 = jnp.bfloat16

softcap = 50.0
epsilon = 1e-06
score_scale = (D // HEADS) ** (-0.5)


def rope_tables():
    half = HD // 2
    freq = np.exp(-np.arange(half, dtype=np.float64) * (2.0 * math.log(10000.0) / HD))
    angles = np.arange(SEQ, dtype=np.float64)[:, None] * freq[None, :]
    cosine, sine = np.cos(angles), np.sin(angles)
    return (
        np.concatenate([cosine, cosine], axis=1).astype(np.float32),
        np.concatenate([-sine, sine], axis=1).astype(np.float32),
    )


def rotate(v, cosine, sine):
    return v * cosine + pltpu.roll(v, HD // 2, 1) * sine


def unrotate(v, cosine, sine):
    return v * cosine - pltpu.roll(v, HD // 2, 1) * sine


def dot_nn(a, b):
    return lax.dot_general(a, b, (((1,), (0,)), ((), ())), preferred_element_type=F32)


def dot_nt(a, b):
    return lax.dot_general(a, b, (((1,), (1,)), ((), ())), preferred_element_type=F32)


def dot_tn(a, b):
    return lax.dot_general(a, b, (((0,), (0,)), ((), ())), preferred_element_type=F32)


def whole(shape):
    return pl.BlockSpec(shape, lambda *_: (0,) * len(shape), pipeline_mode=pl.Buffered(1))


def at_layer(l, shape):
    return pl.BlockSpec(
        (None, *shape), lambda *_: (l, *(0,) * len(shape)), pipeline_mode=pl.Buffered(1)
    )


def forward_kernel(x, gain, wq, wk, wv, cosine, sine, normed, recip, q, kv, wcat):
    rows = x.shape[0]

    @pl.when(pl.program_id(1) == 0)
    def _():
        @pl.loop(0, D // 512)
        def _(c):
            at = pl.ds(pl.multiple_of(c * 512, 512), 512)
            wcat[at, :HD] = wq[at, :]
            wcat[at, HD:] = jnp.concatenate([wk[at, :], wv[at, :]], axis=1)

    @pl.loop(0, rows // 16)
    def _(r):
        at = pl.ds(pl.multiple_of(r * 16, 16), 16)
        v = x[at, :].astype(F32)
        rc = lax.rsqrt(jnp.sum(v * v, axis=1, keepdims=True) * (1.0 / D) + epsilon)
        normed[at, :] = (v * rc * gain[...]).astype(BF16)
        recip[at, :] = jnp.broadcast_to(rc, (16, HD))

    acc = jnp.zeros((rows, 2 * HD), F32)
    for c in range(3):
        at = slice(c * 1536, (c + 1) * 1536)
        acc = acc + dot_nn(normed[:, at], wcat[at, :])
    q[...] = rotate(acc[:, :HD], cosine[...], sine[...]).astype(BF16)
    kv[...] = acc[:, HD:]


def forward(x, gain, wq, wk, wv, cosine, sine):
    br = 192
    row = lambda l, r: (l, r, 0)
    per_layer = lambda l, r: (l, 0, 0)
    return pl.pallas_call(
        forward_kernel,
        grid=(LAYERS, SEQ // br),
        in_specs=[
            pl.BlockSpec((None, br, D), row),
            pl.BlockSpec((None, 1, D), per_layer),
            pl.BlockSpec((None, D, HD), per_layer),
            pl.BlockSpec((None, D, HD // 2), per_layer),
            pl.BlockSpec((None, D, HD // 2), per_layer),
            pl.BlockSpec((br, HD), lambda l, r: (r, 0)),
            pl.BlockSpec((br, HD), lambda l, r: (r, 0)),
        ],
        out_specs=[
            pl.BlockSpec((None, br, D), row),
            pl.BlockSpec((None, br, HD), row),
            pl.BlockSpec((None, br, HD), row),
            pl.BlockSpec((None, br, HD), row),
            pl.BlockSpec((None, D, 2 * HD), per_layer),
        ],
        out_shape=[
            jax.ShapeDtypeStruct((LAYERS, SEQ, D), BF16),
            jax.ShapeDtypeStruct((LAYERS, SEQ, HD), F32),
            jax.ShapeDtypeStruct((LAYERS, SEQ, HD), BF16),
            jax.ShapeDtypeStruct((LAYERS, SEQ, HD), F32),
            jax.ShapeDtypeStruct((LAYERS, D, 2 * HD), BF16),
        ],
        compiler_params=pltpu.CompilerParams(vmem_limit_bytes=48 * 1024 * 1024),
        name="projections",
    )(x, gain.reshape(LAYERS, 1, D), wq, wk, wv, cosine, sine)


def attention_kernel(
    l, lengths, reach, g, wo, q, own, other, cosine, sine, dq_out, keep_out, send_out, att_out
):
    even = lax.axis_index(Z) % 2 == 0
    lane = lax.broadcasted_iota(jnp.int32, (SEQ, HD), 1)
    low = lane < HD // 2
    cs, sn = cosine[...], sine[...]
    first = jnp.where(even, own[...], other[...])
    second = jnp.where(even, other[...], own[...])
    k_raw = jnp.where(low, first, pltpu.roll(second, HD // 2, 1))
    v_raw = jnp.where(low, pltpu.roll(first, HD // 2, 1), second)
    k = rotate(k_raw, cs, sn).astype(BF16)
    v = v_raw.astype(BF16)

    e0 = lengths[0, 0]
    e1 = e0 + lengths[0, 1]
    e2 = e1 + lengths[0, 2]
    span = reach[l]

    def doc(pos):
        return (
            (pos >= e0).astype(jnp.int32)
            + (pos >= e1).astype(jnp.int32)
            + (pos >= e2).astype(jnp.int32)
        )

    i = lax.broadcasted_iota(jnp.int32, (SEQ, SEQ), 0)
    j = lax.broadcasted_iota(jnp.int32, (SEQ, SEQ), 1)
    doc_i = doc(lax.broadcasted_iota(jnp.int32, (SEQ, 1), 0))
    doc_j = doc(lax.broadcasted_iota(jnp.int32, (1, SEQ), 1))
    allowed = (doc_i == doc_j) & (j <= i) & (i - j < span)

    qq = q[...]
    squashed = jnp.tanh(dot_nt(qq, k) * (score_scale / softcap))
    raised = jnp.where(allowed, jnp.exp(softcap * squashed), 0.0)
    prob = raised / jnp.sum(raised, axis=1, keepdims=True)
    rounded = prob.astype(BF16)
    att = dot_nn(rounded, v).astype(BF16)
    ga = jnp.zeros((SEQ, HD), F32)
    for c in range(3):
        at = slice(c * 1536, (c + 1) * 1536)
        ga = ga + dot_nt(g[:, at], wo[:, at])
    ga = ga.astype(BF16)
    delta = jnp.sum(ga.astype(F32) * att.astype(F32), axis=1, keepdims=True)
    ds = prob * (dot_nt(ga, v) - delta) * (1.0 - squashed * squashed) * score_scale
    ds = ds.astype(BF16)
    dq = unrotate(dot_nn(ds, k), cs, sn)
    dk = unrotate(dot_tn(ds, qq), cs, sn)
    dv = dot_tn(rounded, ga)
    dk_turned, dv_turned = pltpu.roll(dk, HD // 2, 1), pltpu.roll(dv, HD // 2, 1)
    lower = jnp.where(low, dk, dv_turned)
    upper = jnp.where(low, dk_turned, dv)
    dq_out[...] = dq.astype(BF16)
    keep_out[...] = jnp.where(even, lower, upper).astype(BF16)
    send_out[...] = jnp.where(even, upper, lower).astype(BF16)
    att_out[...] = att


def attention(l, lengths, reach, g, wo, q, own, other, cosine, sine):
    smem = pl.BlockSpec(memory_space=pltpu.SMEM)
    small = jax.ShapeDtypeStruct((SEQ, HD), BF16)
    return pl.pallas_call(
        functools.partial(attention_kernel, l),
        grid=(1,),
        in_specs=[
            smem,
            smem,
            whole((SEQ, D)),
            at_layer(l, (HD, D)),
            at_layer(l, (SEQ, HD)),
            at_layer(l, (SEQ, HD)),
            at_layer(l, (SEQ, HD)),
            whole((SEQ, HD)),
            whole((SEQ, HD)),
        ],
        out_specs=[whole((SEQ, HD))] * 4,
        out_shape=[small] * 4,
        compiler_params=pltpu.CompilerParams(vmem_limit_bytes=48 * 1024 * 1024),
        name=f"attention{l}",
    )(lengths, reach, g, wo, q, own, other, cosine, sine)


def add(*parts):
    return functools.reduce(lambda a, b: a + b, [p[...].astype(F32) for p in parts])


class Ring:
    def __init__(self, axis, src, bufs, ss, rs):
        i = lax.axis_index(axis)
        up, dn, far = lax.rem(i + 1, 4), lax.rem(i + 3, 4), lax.rem(i + 2, 4)
        r1p, r1m, r2p, r2m, r3p, r3m, tp, tm = bufs
        plan = [
            (src(far, 0), r1p, up),
            (src(far, 1), r1m, dn),
            (src(up, 1), r2p, up),
            (src(dn, 0), r2m, dn),
            (tp, r3p, up),
            (tm, r3m, dn),
        ]
        self.copies = [
            pltpu.make_async_remote_copy(
                src_ref=s,
                dst_ref=d,
                send_sem=ss.at[n],
                recv_sem=rs.at[n],
                device_id={axis: to},
                device_id_type=MESH,
            )
            for n, (s, d, to) in enumerate(plan)
        ]
        self.i, self.up, self.dn, self.src, self.bufs = i, up, dn, src, bufs

    def start(self):
        for n in range(4):
            self.copies[n].start()

    def middle(self):
        r1p, r1m, _, _, _, _, tp, tm = self.bufs
        self.copies[0].wait_recv()
        tp[...] = add(r1p, self.src(self.up, 0)).astype(BF16)
        self.copies[4].start()
        self.copies[1].wait_recv()
        tm[...] = add(r1m, self.src(self.dn, 1)).astype(BF16)
        self.copies[5].start()

    def finish(self, out):
        _, _, r2p, r2m, r3p, r3m, _, _ = self.bufs
        self.copies[3].wait_recv()
        self.copies[4].wait_recv()
        out(0)[...] = add(self.src(self.i, 0), r3p, r2m).astype(BF16)
        self.copies[2].wait_recv()
        self.copies[5].wait_recv()
        out(1)[...] = add(self.src(self.i, 1), r2p, r3m).astype(BF16)

    def drain(self):
        for c in self.copies:
            c.wait_send()


def exchange_kernel(
    last,
    dq,
    keep,
    send,
    att,
    wcat_hbm,
    normed_hbm,
    g_hbm,
    x_hbm,
    recip,
    gain,
    gain_before,
    g_out,
    dw_out,
    gain_out,
    wcat,
    normed,
    g,
    S,
    T,
    dqkv_t,
    att_t,
    dqkv,
    pair_in,
    x_own,
    a1,
    b1,
    a2,
    b2,
    ua,
    ub,
    va,
    x_in,
    stat_out,
    stat_in,
    core_in,
    xl_out,
    xl_in,
    pack,
    gain_in,
    gain_z,
    gain_y,
    s_pair,
    s_local,
    s_a1,
    s_b1,
    s_a2,
    s_b2,
    s_x,
    s_stat,
    s_core,
    s_xl,
    s_g1,
    s_g2,
    s_g3,
    s_ag_x,
    s_ag,
):
    xl, core, y, xh, z = (lax.axis_index(a) for a in (XL, CORE, Y, XH, Z))

    def remote(src, dst, sems, n, **to):
        return pltpu.make_async_remote_copy(
            src_ref=src,
            dst_ref=dst,
            send_sem=sems.at[0, n],
            recv_sem=sems.at[1, n],
            device_id=to,
            device_id_type=MESH,
        )

    ymates = [{Y: lax.rem(y + k, 4)} for k in (1, 2, 3)]
    zmates = [{Z: lax.rem(z + k, 4)} for k in (1, 2, 3)]
    xmates = [
        {XL: lax.rem(xl + a, 2), CORE: lax.rem(core + b, 2), XH: lax.rem(xh + c, 2)}
        for a in (0, 1)
        for b in (0, 1)
        for c in (0, 1)
        if a + b + c
    ]

    l = 0 if last else 1
    fetch = [
        pltpu.make_async_copy(src, dst, s_local.at[n])
        for n, (src, dst) in enumerate(
            [
                (wcat_hbm.at[l], wcat),
                (normed_hbm.at[l], normed),
                (g_hbm, g),
                (x_hbm.at[l, pl.ds(z * 96 + xh * RB, RB), pl.ds(y * CB, CB)], x_own),
            ]
        )
    ]
    for c in fetch:
        c.start()

    barrier = pltpu.get_barrier_semaphore()
    for to in (*ymates, *zmates, *xmates):
        pl.semaphore_signal(barrier, inc=1, device_id=to, device_id_type=MESH)
    pl.semaphore_wait(barrier, 13)

    pair = remote(send, pair_in, s_pair, 0, **{Z: z + 1 - 2 * lax.rem(z, 2)})
    pair.start()
    dqkv[:, :HD] = dq[...]
    pair.wait_recv()
    dqkv[:, HD:] = add(keep, pair_in).astype(BF16)

    fetch[0].wait()

    @pl.loop(0, D // 512)
    def _(c):
        at = pl.ds(pl.multiple_of(c * 512, 512), 512)
        S[:, :, :, at] = dot_nt(dqkv[...], wcat[at, :]).astype(BF16).reshape(4, 2, RB, 512)

    def cols(t, width=CB, shift=0):
        return pl.ds(pl.multiple_of(t * CB + shift, 128), width)

    ring_a1 = Ring(
        Y,
        lambda t, h: S.at[pl.ds(2 * h, 2), 0, :, cols(t)],
        [a1.at[n] for n in range(8)],
        s_a1.at[0],
        s_a1.at[1],
    )
    ring_b1 = Ring(
        Z,
        lambda t, h: S.at[t, 1, :, pl.ds(h * 2 * CB, 2 * CB)],
        [b1.at[n] for n in range(8)],
        s_b1.at[0],
        s_b1.at[1],
    )
    part = [pl.ds(0, CA), pl.ds(CA, CB - CA)]
    kinds = (0, 1, 1, 0, 0, 1, 0, 1)
    ring_a2 = Ring(
        Z,
        lambda t, h: ua.at[t, :, part[h]],
        [a2.at[n, :, part[h]] for n, h in enumerate(kinds)],
        s_a2.at[0],
        s_a2.at[1],
    )
    ring_b2 = Ring(
        Y,
        lambda t, h: ub.at[:, cols(t, (CA, CB - CA)[h], h * CA)],
        [b2.at[n, :, part[h]] for n, h in enumerate(kinds)],
        s_b2.at[0],
        s_b2.at[1],
    )
    ring_a1.start()
    ring_b1.start()

    dqkv_t[...] = dqkv[...].T
    att_t[...] = att[...].T
    fetch[1].wait()
    fetch[2].wait()

    @pl.loop(0, D // 512)
    def _(c):
        at = pl.ds(pl.multiple_of(c * 512, 512), 512)
        T[: 2 * HD, at] = dot_nn(dqkv_t[...], normed[:, at]).astype(BF16)
        T[2 * HD :, at] = dot_nn(att_t[...], g[:, at]).astype(BF16)

    to_core = [
        remote(
            T.at[:, pl.ds(pl.multiple_of((2 * k + 1 - core) * CB, 128), CB)],
            core_in.at[k],
            s_core,
            k,
            **{CORE: 1 - core},
        )
        for k in (0, 1)
    ]
    to_core[0].start()
    to_core[1].start()

    ring_a1.middle()
    ring_b1.middle()
    ring_a1.finish(lambda h: ua.at[pl.ds(2 * h, 2)])
    ring_a2.start()
    ring_b1.finish(lambda h: ub.at[:, pl.ds(h * 2 * CB, 2 * CB)])
    ring_b2.start()
    ring_a2.middle()
    ring_b2.middle()
    ring_a2.finish(lambda h: va.at[0, :, part[h]])
    ring_b2.finish(lambda h: va.at[1, :, part[h]])
    to_x = remote(va.at[1 - xh], x_in, s_x, 0, **{XH: 1 - xh})
    to_x.start()

    for c in to_core:
        c.wait_recv()

    def dp_cols(k):
        return pl.ds(pl.multiple_of((2 * k + core) * CB, 128), CB)

    @pl.loop(0, SEQ // 32)
    def _(r):
        at = pl.ds(pl.multiple_of(r * 32, 32), 32)
        there = T[at, dp_cols(1 - xl)].astype(F32) + core_in[1 - xl, at, :].astype(F32)
        xl_out[at, :] = there.astype(BF16)

    fetch[3].wait()
    to_x.wait_recv()
    grad = add(va.at[xh], x_in)
    rows = pl.ds(pl.multiple_of(z * 96 + xh * RB, 16), RB)
    rc = recip[rows, :][:, :1]
    gn = gain[:, cols(y)]
    unit = x_own[...].astype(F32) * rc
    u = grad * gn
    stat = jnp.sum(u * unit, axis=1, keepdims=True)
    stat_out[...] = jnp.broadcast_to(stat, (RB, HD))
    to_stat = [remote(stat_out, stat_in.at[n], s_stat, n, **to) for n, to in enumerate(ymates)]
    for c in to_stat:
        c.start()
    per_feature = jnp.sum(grad * unit, axis=0, keepdims=True)
    pack[...] = gain_before[...]
    for n in range(9):
        k = n + 9 if last else n
        pack[k : k + 1, :] = per_feature[:, n * 128 : (n + 1) * 128]
    if last:
        to_g1 = [remote(pack, gain_in.at[n], s_g1, n, **to) for n, to in enumerate(xmates)]
        for c in to_g1:
            c.start()
    else:
        gain_out[...] = pack[...]
    for c in to_stat:
        c.wait_recv()
    mean = (stat_out[...] + stat_in[0] + stat_in[1] + stat_in[2])[:, :1] * (1.0 / D)
    up_own = g[rows, cols(y)].astype(F32)
    g_out[z, xh, :, cols(y)] = (up_own + rc * (u - unit * mean)).astype(BF16)

    def spread(zz, hh, yy, shift, width, n, **to):
        ref = g_out.at[zz, hh, :, cols(yy, width, shift)]
        return remote(ref, ref, s_ag, n, **to)

    def walk(first_axis, hh, base):
        second = Y if first_axis == Z else Z
        i, j = (z, y) if first_axis == Z else (y, z)
        order = [i, lax.rem(i + 3, 4), lax.rem(i + 1, 4), lax.rem(i + 2, 4)]
        up1, dn1 = {first_axis: lax.rem(i + 1, 4)}, {first_axis: lax.rem(i + 3, 4)}
        up2, dn2 = {second: lax.rem(j + 1, 4)}, {second: lax.rem(j + 3, 4)}
        jdn, jup, jfar = lax.rem(j + 3, 4), lax.rem(j + 1, 4), lax.rem(j + 2, 4)

        def one(ii, jj, n, to, shift=0, width=CB):
            zz, yy = (ii, jj) if first_axis == Z else (jj, ii)
            return spread(zz, hh, yy, shift, width, base + n, **to)

        sent = []

        def go(c):
            c.start()
            sent.append(c)

        def begin():
            go(one(order[0], j, 0, up1))
            go(one(order[0], j, 1, dn1))
            go(one(order[0], j, 4, up2))
            go(one(order[0], j, 5, dn2))

        def arrive_dn():
            one(order[1], j, 0, up1).wait_recv()
            go(one(order[1], j, 2, up1, 0, CA))
            go(one(order[1], j, 6, up2))
            go(one(order[1], j, 7, dn2))

        def arrive_up():
            one(order[2], j, 1, dn1).wait_recv()
            go(one(order[2], j, 3, dn1, CA, CB - CA))
            go(one(order[2], j, 8, up2))
            go(one(order[2], j, 9, dn2))

        def arrive_far():
            one(order[3], j, 2, up1, 0, CA).wait_recv()
            one(order[3], j, 3, dn1, CA, CB - CA).wait_recv()
            go(one(order[3], j, 10, up2))
            go(one(order[3], j, 11, dn2))

        def second_step(k):
            one(order[k], jdn, 4 + 2 * k, up2).wait_recv()
            if k in (0, 2):
                go(one(order[k], jdn, 12 + k, up2))
            one(order[k], jup, 5 + 2 * k, dn2).wait_recv()
            if k in (1, 3):
                go(one(order[k], jup, 12 + k, dn2))

        def last_step(k):
            one(order[k], jfar, 12 + k, up2 if k in (0, 2) else dn2).wait_recv()

        def done():
            for c in sent:
                c.wait_send()

        return begin, arrive_dn, arrive_up, arrive_far, second_step, last_step, done

    mine = g_out.at[z, xh, :, cols(y)]
    across = remote(mine, mine, s_ag_x, 0, **{XH: 1 - xh})
    across.start()
    own = walk(Z, xh, 0)
    oth = walk(Y, 1 - xh, 16)
    own[0]()
    to_xl = remote(xl_out, xl_in, s_xl, 0, **{XL: 1 - xl})
    to_xl.start()
    own[1]()
    own[2]()
    theirs = g_out.at[z, 1 - xh, :, cols(y)]
    remote(theirs, theirs, s_ag_x, 0, **{XH: 1 - xh}).wait_recv()
    oth[0]()
    own[4](0)
    own[3]()
    oth[1]()
    oth[2]()
    own[4](1)
    oth[4](0)
    own[4](2)
    oth[3]()
    oth[4](1)
    if last:
        for c in to_g1:
            c.wait_recv()
        total = pack[...]
        for n in range(7):
            total = total + gain_in[n]
        gain_in[7] = total
        to_g2 = [remote(gain_in.at[7], gain_z.at[n], s_g2, n, **t) for n, t in enumerate(zmates)]
        for c in to_g2:
            c.start()
    own[4](3)
    oth[4](2)
    if last:
        for c in to_g2:
            c.wait_recv()
        total = (gain_in[7] + gain_z[0] + gain_z[1] + gain_z[2]) * (1.0 / 4)
        gain_z[3] = total
        to_g3 = [remote(gain_z.at[3], gain_y.at[n], s_g3, n, **t) for n, t in enumerate(ymates)]
        for c in to_g3:
            c.start()
    oth[4](3)
    for k in range(4):
        own[5](k)
        oth[5](k)
    if last:
        for c in to_g3:
            c.wait_recv()
        for n in range(-1, 3):
            ref = gain_z.at[3] if n < 0 else gain_y.at[n]
            yy = lax.rem(y + 3 - n, 4)
            for k in range(9):
                at = pl.ds(pl.multiple_of(yy * CB + k * 128, 128), 128)
                gain_out[1:2, at] = ref[k : k + 1, :]
                gain_out[0:1, at] = ref[9 + k : 10 + k, :]

    to_xl.wait_recv()

    @pl.loop(0, SEQ // 32)
    def _(r):
        at = pl.ds(pl.multiple_of(r * 32, 32), 32)
        here = T[at, dp_cols(xl)].astype(F32) + core_in[xl, at, :].astype(F32)
        dw_out[at, :] = (here + xl_in[at, :].astype(F32)) * (1.0 / 4)

    pair.wait_send()
    for ring in (ring_a1, ring_b1, ring_a2, ring_b2):
        ring.drain()
    to_x.wait_send()
    across.wait_send()
    to_xl.wait_send()
    for c in (*to_core, *to_stat):
        c.wait_send()
    if last:
        for c in (*to_g1, *to_g2, *to_g3):
            c.wait_send()
    own[6]()
    oth[6]()


def exchange(l, dq, keep, send, att, wcat, normed, g, x, recip, gain, gain_before):
    last = l == 0
    sem = pltpu.SemaphoreType.DMA
    gain_shape = (8, D) if last else (24, 128)
    hbm = pl.BlockSpec(memory_space=pl.ANY)
    return pl.pallas_call(
        functools.partial(exchange_kernel, last),
        grid=(1,),
        in_specs=[
            whole((SEQ, HD)),
            whole((SEQ, HD)),
            whole((SEQ, HD)),
            whole((SEQ, HD)),
            hbm,
            hbm,
            hbm,
            hbm,
            at_layer(l, (SEQ, HD)),
            at_layer(l, (1, D)),
            whole((24, 128)),
        ],
        out_specs=[whole((4, 2, RB, D)), whole((SEQ, CB)), whole(gain_shape)],
        out_shape=[
            jax.ShapeDtypeStruct((4, 2, RB, D), BF16),
            jax.ShapeDtypeStruct((SEQ, CB), F32),
            jax.ShapeDtypeStruct(gain_shape, F32),
        ],
        scratch_shapes=[
            VMEM((D, 2 * HD), BF16),
            VMEM((SEQ, D), BF16),
            VMEM((SEQ, D), BF16),
            VMEM((4, 2, RB, D), BF16),
            VMEM((SEQ, D), BF16),
            VMEM((2 * HD, SEQ), BF16),
            VMEM((HD, SEQ), BF16),
            VMEM((SEQ, 2 * HD), BF16),
            VMEM((SEQ, HD), BF16),
            VMEM((RB, CB), BF16),
            VMEM((8, 2, RB, CB), BF16),
            VMEM((8, RB, 2 * CB), BF16),
            VMEM((8, RB, CB), BF16),
            VMEM((8, RB, CB), BF16),
            VMEM((4, RB, CB), BF16),
            VMEM((RB, D), BF16),
            VMEM((2, RB, CB), BF16),
            VMEM((RB, CB), BF16),
            VMEM((RB, HD), F32),
            VMEM((3, RB, HD), F32),
            VMEM((2, SEQ, CB), BF16),
            VMEM((SEQ, CB), BF16),
            VMEM((SEQ, CB), BF16),
            VMEM((24, 128), F32),
            VMEM((8, 24, 128), F32),
            VMEM((4, 24, 128), F32),
            VMEM((3, 24, 128), F32),
            sem((2, 1)),
            sem((4,)),
            sem((2, 6)),
            sem((2, 6)),
            sem((2, 6)),
            sem((2, 6)),
            sem((2, 1)),
            sem((2, 3)),
            sem((2, 2)),
            sem((2, 1)),
            sem((2, 7)),
            sem((2, 3)),
            sem((2, 3)),
            sem((2, 1)),
            sem((2, 32)),
        ],
        compiler_params=pltpu.CompilerParams(
            collective_id=l, has_side_effects=True, vmem_limit_bytes=62 * 1024 * 1024
        ),
        name=f"exchange{l}",
    )(
        dq,
        keep,
        send,
        att,
        wcat,
        normed,
        g,
        x,
        recip,
        gain.reshape(LAYERS, 1, D),
        gain_before,
    )


def local(layer_inputs, out_grad, gain, w_query, w_key, w_value, w_out, doc_lengths, window_reach):
    cosine, sine = (jnp.asarray(t) for t in rope_tables())
    normed, recip, q, kv, wcat = forward(
        layer_inputs, gain, w_query, w_key, w_value, cosine, sine
    )
    kv_other = lax.ppermute(kv, Z, [(i, i ^ 1) for i in range(4)])
    g = out_grad
    gains = jnp.zeros((24, 128), F32)
    grads = [None] * LAYERS
    for l in reversed(range(LAYERS)):
        dq, keep, send, att = attention(
            l, doc_lengths, window_reach, g, w_out, q, kv, kv_other, cosine, sine
        )
        g, grads[l], gains = exchange(
            l, dq, keep, send, att, wcat, normed, g, layer_inputs, recip, gain, gains
        )
        g = g.reshape(SEQ, D)
    grads = jnp.stack(grads)
    qkv = jnp.swapaxes(grads[:, : 2 * HD], 1, 2)
    return (
        g,
        qkv[:, :, :HD],
        qkv[:, :, HD : HD + HD // 2],
        qkv[:, :, HD + HD // 2 :],
        grads[:, 2 * HD :],
        gains[:LAYERS],
    )


def solution(mesh):
    split = Mesh(mesh.devices.reshape(2, 2, 4, 2, 4), (XL, CORE, Y, XH, Z))
    in_specs = (
        P(None, DP, None),
        P(DP, None),
        P(),
        P(None, None, TP),
        P(None, None, TP),
        P(None, None, TP),
        P(None, TP, None),
        P(DP, None),
        P(),
    )
    out_specs = (
        P(DP, None),
        P(None, DP, TP),
        P(None, DP, TP),
        P(None, DP, TP),
        P(None, TP, DP),
        P(),
    )
    return jax.shard_map(local, mesh=split, in_specs=in_specs, out_specs=out_specs, check_vma=False)
```

```python
import functools
import math

import jax
import jax.numpy as jnp
import numpy as np
from jax import lax
from jax.experimental import pallas as pl
from jax.experimental.pallas import tpu as pltpu
from jax.sharding import Mesh
from jax.sharding import PartitionSpec as P

D = 4608
HEADS = 32
HD = 128
SEQ = 384
LAYERS = 2
CB = D // 4
RB = 48
CA = 640
XL, CORE, Y, XH, Z = ("dp_0", "dp_1", "tp_0", "tp_1", "tp_2")
TP = (Y, XH, Z)
DP = (XL, CORE)
MESH = pl.DeviceIdType.MESH
VMEM = pltpu.VMEM
F32 = jnp.float32
BF16 = jnp.bfloat16
VMEM_LIMIT = 54 * 1024 * 1024

softcap = 50.0
epsilon = 1e-06
score_scale = (D // HEADS) ** (-0.5)


def rope_tables():
    half = HD // 2
    freq = np.exp(-np.arange(half, dtype=np.float64) * (2.0 * math.log(10000.0) / HD))
    angles = np.arange(SEQ, dtype=np.float64)[:, None] * freq[None, :]
    cosine, sine = np.cos(angles), np.sin(angles)
    return (
        np.concatenate([cosine, cosine], axis=1).astype(np.float32),
        np.concatenate([-sine, sine], axis=1).astype(np.float32),
    )


def rotate(v, cosine, sine):
    return v * cosine + pltpu.roll(v, HD // 2, 1) * sine


def unrotate(v, cosine, sine):
    return v * cosine - pltpu.roll(v, HD // 2, 1) * sine


def dot_nn(a, b):
    return lax.dot_general(a, b, (((1,), (0,)), ((), ())), preferred_element_type=F32)


def dot_nt(a, b):
    return lax.dot_general(a, b, (((1,), (1,)), ((), ())), preferred_element_type=F32)


def dot_tn(a, b):
    return lax.dot_general(a, b, (((0,), (0,)), ((), ())), preferred_element_type=F32)


def add(*parts):
    return functools.reduce(lambda a, b: a + b, [p[...].astype(F32) for p in parts])


class Ring:
    def __init__(self, axis, src, bufs, ss, rs):
        i = lax.axis_index(axis)
        up, dn, far = lax.rem(i + 1, 4), lax.rem(i + 3, 4), lax.rem(i + 2, 4)
        r1p, r1m, r2p, r2m, r3p, r3m, tp, tm = bufs
        plan = [
            (src(far, 0), r1p, up),
            (src(far, 1), r1m, dn),
            (src(up, 1), r2p, up),
            (src(dn, 0), r2m, dn),
            (tp, r3p, up),
            (tm, r3m, dn),
        ]
        self.copies = [
            pltpu.make_async_remote_copy(
                src_ref=s,
                dst_ref=d,
                send_sem=ss.at[n],
                recv_sem=rs.at[n],
                device_id={axis: to},
                device_id_type=MESH,
            )
            for n, (s, d, to) in enumerate(plan)
        ]
        self.i, self.up, self.dn, self.src, self.bufs = i, up, dn, src, bufs

    def start(self, which):
        for n in which:
            self.copies[n].start()

    def middle(self):
        r1p, r1m, _, _, _, _, tp, tm = self.bufs
        self.copies[0].wait_recv()
        tp[...] = add(r1p, self.src(self.up, 0)).astype(BF16)
        self.copies[4].start()
        self.copies[1].wait_recv()
        tm[...] = add(r1m, self.src(self.dn, 1)).astype(BF16)
        self.copies[5].start()

    def finish(self, out):
        _, _, r2p, r2m, r3p, r3m, _, _ = self.bufs
        self.copies[3].wait_recv()
        self.copies[4].wait_recv()
        out(0)[...] = add(self.src(self.i, 0), r3p, r2m).astype(BF16)
        self.copies[2].wait_recv()
        self.copies[5].wait_recv()
        out(1)[...] = add(self.src(self.i, 1), r2p, r3m).astype(BF16)

    def drain(self):
        for c in self.copies:
            c.wait_send()


def write_kernel(*refs):
    *refs, sems = refs
    n = len(refs) // 2
    copies = [pltpu.make_async_copy(refs[k], refs[n + k], sems.at[k]) for k in range(n)]
    for c in copies:
        c.start()
    for c in copies:
        c.wait()


def write_out(*arrays):
    arrays = [pltpu.with_memory_space_constraint(a, pltpu.VMEM) for a in arrays]
    return pl.pallas_call(
        write_kernel,
        in_specs=[pl.BlockSpec(memory_space=pltpu.VMEM)] * len(arrays),
        out_specs=[pl.BlockSpec(memory_space=pl.ANY)] * len(arrays),
        out_shape=[jax.ShapeDtypeStruct(a.shape, a.dtype) for a in arrays],
        scratch_shapes=[pltpu.SemaphoreType.DMA((len(arrays),))],
        compiler_params=pltpu.CompilerParams(vmem_limit_bytes=1024 * 1024),
        name="write_out",
    )(*arrays)


def step_kernel(
    lengths,
    reach,
    x_hbm,
    g_hbm,
    gain,
    wq_hbm,
    wk_hbm,
    wv_hbm,
    wo_hbm,
    cosine,
    sine,
    g_out,
    dwq,
    dwk,
    dwv,
    dwo,
    gain_out,
    m,
):
    xl, core, y, xh, z = (lax.axis_index(a) for a in (XL, CORE, Y, XH, Z))
    half = HD // 2

    def remote(src, dst, sems, n, **to):
        return pltpu.make_async_remote_copy(
            src_ref=src,
            dst_ref=dst,
            send_sem=sems.at[0, n],
            recv_sem=sems.at[1, n],
            device_id=to,
            device_id_type=MESH,
        )

    def rows_of(zz, hh):
        return pl.ds(pl.multiple_of(zz * 96 + hh * RB, 16), RB)

    def cols(t, width=CB, shift=0):
        return pl.ds(pl.multiple_of(t * CB + shift, 128), width)

    ymates = [{Y: lax.rem(y + k, 4)} for k in (1, 2, 3)]
    zmates = [{Z: lax.rem(z + k, 4)} for k in (1, 2, 3)]
    xmates = [
        {XL: lax.rem(xl + a, 2), CORE: lax.rem(core + b, 2), XH: lax.rem(xh + c, 2)}
        for a in (0, 1)
        for b in (0, 1)
        for c in (0, 1)
        if a + b + c
    ]
    pair = {Z: z + 1 - 2 * lax.rem(z, 2)}
    even = lax.rem(z, 2) == 0

    def fetch(n, src, dst):
        return pltpu.make_async_copy(src, dst, m["s_local"].at[n])

    get_x, get_wkv, get_wq, get_wo, get_own = {}, {}, {}, {}, {}
    for l in (1, 0):
        get_x[l] = [
            fetch(16 * l + c, x_hbm.at[l, pl.ds(c * 96, 96)], m["x"].at[c % 2])
            for c in range(4)
        ]
        get_wkv[l] = [
            fetch(16 * l + 4, wk_hbm.at[l], m["wkv"].at[pl.ds(0, half)]),
            fetch(16 * l + 5, wv_hbm.at[l], m["wkv"].at[pl.ds(half, half)]),
        ]
        get_wq[l] = fetch(16 * l + 6, wq_hbm.at[l], m["wq"])
        get_wo[l] = fetch(16 * l + 7, wo_hbm.at[l], m["wo"])
        get_own[l] = fetch(16 * l + 8, x_hbm.at[l, rows_of(z, xh), cols(y)], m["x_own"].at[l])
    get_g = fetch(9, g_hbm, m["g0"])
    for c in (*get_x[1][:2], *get_wkv[1], get_wq[1], get_wo[1], get_g, get_own[1]):
        c.start()
    get_own[0].start()

    barrier = pltpu.get_barrier_semaphore()
    for to in (*ymates, *zmates, *xmates):
        pl.semaphore_signal(barrier, inc=1, device_id=to, device_id_type=MESH)

    kv_pair = [remote(m["kv_send"].at[l], m["kv_in"].at[l], m["s_kv"].at[l], 0, **pair) for l in (0, 1)]
    cs, sn = cosine, sine

    def front(l):
        x, normed = m["x"], m["normed"]
        for c in range(4):
            get_x[l][c].wait()

            @pl.loop(0, 6)
            def _(r):
                at = pl.ds(pl.multiple_of(c * 96 + r * 16, 16), 16)
                v = x[c % 2, pl.ds(pl.multiple_of(r * 16, 16), 16), :].astype(F32)
                rc = lax.rsqrt(jnp.sum(v * v, axis=1, keepdims=True) * (1.0 / D) + epsilon)
                normed[at, :] = (v * rc * gain[l : l + 1, :]).astype(BF16)
                m["recip"][l, at, :] = jnp.broadcast_to(rc, (16, HD))

            if c < 2:
                get_x[l][c + 2].start()
            elif l == 1:
                get_x[0][c - 2].start()

        for c in get_wkv[l]:
            c.wait()
        acc = jnp.zeros((SEQ, HD), F32)
        for c in range(3):
            at = slice(c * 1536, (c + 1) * 1536)
            acc = acc + dot_nt(normed[:, at], m["wkv"][:, at])
        m["kv"][...] = acc
        m["kv_send"][l] = acc.astype(BF16)
        if l == 1:
            pl.semaphore_wait(barrier, 13)
        kv_pair[l].start()
        get_wq[l].wait()
        acc = jnp.zeros((SEQ, HD), F32)
        for c in range(3):
            at = slice(c * 1536, (c + 1) * 1536)
            acc = acc + dot_nn(normed[:, at], m["wq"][at, :])
        m["q"][...] = rotate(acc, cs[...], sn[...]).astype(BF16)

    low = lax.broadcasted_iota(jnp.int32, (SEQ, HD), 1) < half

    def attention(l, g):
        if l == 1:
            get_g.wait()
        get_wo[l].wait()
        ga = jnp.zeros((SEQ, HD), F32)
        for c in range(3):
            at = slice(c * 1536, (c + 1) * 1536)
            ga = ga + dot_nt(g[:, at], m["wo"][:, at])
        ga = ga.astype(BF16)

        kv_pair[l].wait_recv()
        own, other = m["kv"][...], m["kv_in"][l].astype(F32)
        first = jnp.where(even, own, other)
        second = jnp.where(even, other, own)
        k_raw = jnp.where(low, first, pltpu.roll(second, half, 1))
        v_raw = jnp.where(low, pltpu.roll(first, half, 1), second)
        k = rotate(k_raw, cs[...], sn[...]).astype(BF16)
        v = v_raw.astype(BF16)

        e0 = lengths[0, 0]
        e1 = e0 + lengths[0, 1]
        e2 = e1 + lengths[0, 2]
        span = reach[l]

        def doc(pos):
            return (
                (pos >= e0).astype(jnp.int32)
                + (pos >= e1).astype(jnp.int32)
                + (pos >= e2).astype(jnp.int32)
            )

        i = lax.broadcasted_iota(jnp.int32, (SEQ, SEQ), 0)
        j = lax.broadcasted_iota(jnp.int32, (SEQ, SEQ), 1)
        doc_i = doc(lax.broadcasted_iota(jnp.int32, (SEQ, 1), 0))
        doc_j = doc(lax.broadcasted_iota(jnp.int32, (1, SEQ), 1))
        allowed = (doc_i == doc_j) & (j <= i) & (i - j < span)

        q = m["q"][...]
        squashed = jnp.tanh(dot_nt(q, k) * (score_scale / softcap))
        raised = jnp.where(allowed, jnp.exp(softcap * squashed), 0.0)
        prob = raised / jnp.sum(raised, axis=1, keepdims=True)
        rounded = prob.astype(BF16)
        att = dot_nn(rounded, v).astype(BF16)
        delta = jnp.sum(ga.astype(F32) * att.astype(F32), axis=1, keepdims=True)
        ds = prob * (dot_nt(ga, v) - delta) * (1.0 - squashed * squashed) * score_scale
        ds = ds.astype(BF16)
        dk = unrotate(dot_tn(ds, q), cs[...], sn[...])
        dv = dot_tn(rounded, ga)
        lower = jnp.where(low, dk, pltpu.roll(dv, half, 1))
        upper = jnp.where(low, pltpu.roll(dk, half, 1), dv)
        m["keep"][...] = jnp.where(even, lower, upper).astype(BF16)
        m["send"][l] = jnp.where(even, upper, lower).astype(BF16)
        dkv_pair[l].start()
        dq = unrotate(dot_nn(ds, k), cs[...], sn[...]).astype(BF16)
        m["dq"][...] = dq
        m["dq_t"][...] = dq.T
        m["att_t"][...] = att.T

    dkv_pair = [remote(m["send"].at[l], m["dkv_in"].at[l], m["s_dkv"].at[l], 0, **pair) for l in (0, 1)]

    S, T = m["S"], m["T"]
    part = [pl.ds(0, CA), pl.ds(CA, CB - CA)]
    kinds = (0, 1, 1, 0, 0, 1, 0, 1)

    def dp_cols(k):
        return pl.ds(pl.multiple_of((2 * k + core) * CB, 128), CB)

    def finish_weights(l, to_xl):
        to_xl.wait_recv()

        @pl.loop(0, 9)
        def _(k):
            at = pl.ds(pl.multiple_of(k * 128, 128), 128)
            v = (m["dw"][:, at] + m["xl_in"][l, :, at].astype(F32)) * (1.0 / 4)
            dwq[l, at, :] = v[:HD].T
            dwk[l, :, at] = v[HD : HD + half]
            dwv[l, :, at] = v[HD + half : 2 * HD]
            dwo[l, :, at] = v[2 * HD :]

    front(1)
    pack = m["pack"]
    pack[...] = jnp.zeros((24, 128), F32)
    to_xl = {}
    waiting = []
    for l in (1, 0):
        last = l == 0
        g, to = (m["g1"], g_out) if last else (m["g0"], m["g1"])
        attention(l, g)
        if not last:
            get_wo[0].start()
        normed = m["normed"]

        @pl.loop(0, D // 512)
        def _(c):
            at = pl.ds(pl.multiple_of(c * 512, 512), 512)
            T[:HD, at] = dot_nn(m["dq_t"][...], normed[:, at]).astype(BF16)
            T[2 * HD :, at] = dot_nn(m["att_t"][...], g[:, at]).astype(BF16)

        dkv_pair[l].wait_recv()
        dkv = add(m["keep"], m["dkv_in"].at[l]).astype(BF16)
        m["dkv"][...] = dkv
        m["dkv_t"][...] = dkv.T

        sa1, sb1, sa2, sb2 = (m[n].at[l] for n in ("s_a1", "s_b1", "s_a2", "s_b2"))
        ua, ub, va = m["ua"], m["ub"], m["va"]
        ring_a1 = Ring(
            Y,
            lambda t, h: S.at[pl.ds(2 * h, 2), 0, :, cols(t)],
            [m["a1"].at[n] for n in range(8)],
            sa1.at[0],
            sa1.at[1],
        )
        ring_b1 = Ring(
            Z,
            lambda t, h: S.at[t, 1, :, pl.ds(h * 2 * CB, 2 * CB)],
            [m["b1"].at[n] for n in range(8)],
            sb1.at[0],
            sb1.at[1],
        )
        ring_a2 = Ring(
            Z,
            lambda t, h: ua.at[t, :, part[h]],
            [m["a2"].at[n, :, part[h]] for n, h in enumerate(kinds)],
            sa2.at[0],
            sa2.at[1],
        )
        ring_b2 = Ring(
            Y,
            lambda t, h: ub.at[:, cols(t, (CA, CB - CA)[h], h * CA)],
            [m["b2"].at[n, :, part[h]] for n, h in enumerate(kinds)],
            sb2.at[0],
            sb2.at[1],
        )

        for k, starts in ((2, (0, 1)), (1, (2,)), (3, (3,)), (0, ())):

            @pl.loop(0, 3)
            def _(c):
                at = pl.ds(pl.multiple_of(lax.rem(y + k, 4) * CB + c * 384, 128), 384)
                v = dot_nt(m["dq"][...], m["wq"][at, :])
                v = v + dot_nn(m["dkv"][...], m["wkv"][:, at])
                S[:, :, :, at] = v.astype(BF16).reshape(4, 2, RB, 384)

            ring_a1.start(starts)
        ring_b1.start(range(4))
        if not last:
            for c in (*get_wkv[0], get_wq[0]):
                c.start()

        @pl.loop(0, D // 512)
        def _(c):
            at = pl.ds(pl.multiple_of(c * 512, 512), 512)
            T[HD : 2 * HD, at] = dot_nn(m["dkv_t"][...], normed[:, at]).astype(BF16)

        to_core = [
            remote(
                T.at[:, pl.ds(pl.multiple_of((2 * k + 1 - core) * CB, 128), CB)],
                m["core_in"].at[l, k],
                m["s_core"].at[l],
                k,
                **{CORE: 1 - core},
            )
            for k in (0, 1)
        ]
        to_core[0].start()
        to_core[1].start()

        ring_a1.middle()
        ring_b1.middle()
        if last:
            finish_weights(1, to_xl[1])
        else:
            front(0)
        ring_a1.finish(lambda h: ua.at[pl.ds(2 * h, 2)])
        ring_a2.start(range(4))
        ring_b1.finish(lambda h: ub.at[:, pl.ds(h * 2 * CB, 2 * CB)])
        ring_b2.start(range(4))
        ring_a2.middle()
        ring_b2.middle()
        ring_a2.finish(lambda h: va.at[0, :, part[h]])
        ring_b2.finish(lambda h: va.at[1, :, part[h]])
        to_x = remote(va.at[1 - xh], m["x_in"], m["s_x"].at[l], 0, **{XH: 1 - xh})
        to_x.start()

        for c in to_core:
            c.wait_recv()
        xl_out = m["xl_out"]
        if last:
            to_xl[1].wait_send()

        @pl.loop(0, SEQ // 32)
        def _(r):
            at = pl.ds(pl.multiple_of(r * 32, 32), 32)
            there = T[at, dp_cols(1 - xl)].astype(F32) + m["core_in"][l, 1 - xl, at, :].astype(F32)
            xl_out[at, :] = there.astype(BF16)

        get_own[l].wait()
        to_x.wait_recv()
        rows = rows_of(z, xh)
        grad = add(va.at[xh], m["x_in"])
        rc = m["recip"][l, rows, :][:, :1]
        gn = gain[l : l + 1, cols(y)]
        unit = m["x_own"][l].astype(F32) * rc
        u = grad * gn
        stat = jnp.sum(u * unit, axis=1, keepdims=True)
        m["stat_out"][l] = jnp.broadcast_to(stat, (RB, HD))
        to_stat = [
            remote(m["stat_out"].at[l], m["stat_in"].at[l, n], m["s_stat"].at[l], n, **t)
            for n, t in enumerate(ymates)
        ]
        for c in to_stat:
            c.start()
        per_feature = jnp.sum(grad * unit, axis=0, keepdims=True)
        for n in range(9):
            k = n + 9 if last else n
            pack[k : k + 1, :] = per_feature[:, n * 128 : (n + 1) * 128]
        if last:
            gain_in, gain_z, gain_y = m["gain_in"], m["gain_z"], m["gain_y"]
            to_g1 = [
                remote(pack, gain_in.at[n], m["s_g1"], n, **t) for n, t in enumerate(xmates)
            ]
            for c in to_g1:
                c.start()
        for c in to_stat:
            c.wait_recv()
        total = m["stat_out"][l]
        for n in range(3):
            total = total + m["stat_in"][l, n]
        mean = total[:, :1] * (1.0 / D)
        up_own = g[rows, cols(y)].astype(F32)
        to[rows, cols(y)] = (up_own + rc * (u - unit * mean)).astype(BF16)

        def spread(zz, hh, yy, shift, width, n, dest):
            ref = to.at[rows_of(zz, hh), cols(yy, width, shift)]
            return remote(ref, ref, m["s_ag"].at[l], n, **dest)

        def walk(first_axis, hh, base):
            second = Y if first_axis == Z else Z
            i, j = (z, y) if first_axis == Z else (y, z)
            order = [i, lax.rem(i + 3, 4), lax.rem(i + 1, 4), lax.rem(i + 2, 4)]
            up1, dn1 = {first_axis: lax.rem(i + 1, 4)}, {first_axis: lax.rem(i + 3, 4)}
            up2, dn2 = {second: lax.rem(j + 1, 4)}, {second: lax.rem(j + 3, 4)}
            jdn, jup, jfar = lax.rem(j + 3, 4), lax.rem(j + 1, 4), lax.rem(j + 2, 4)

            def one(ii, jj, n, dest, shift=0, width=CB):
                zz, yy = (ii, jj) if first_axis == Z else (jj, ii)
                return spread(zz, hh, yy, shift, width, base + n, dest)

            sent = []

            def go(c):
                c.start()
                sent.append(c)

            def begin():
                go(one(order[0], j, 0, up1))
                go(one(order[0], j, 1, dn1))
                go(one(order[0], j, 4, up2))
                go(one(order[0], j, 5, dn2))

            def arrive_dn():
                one(order[1], j, 0, up1).wait_recv()
                go(one(order[1], j, 2, up1, 0, CA))
                go(one(order[1], j, 6, up2))
                go(one(order[1], j, 7, dn2))

            def arrive_up():
                one(order[2], j, 1, dn1).wait_recv()
                go(one(order[2], j, 3, dn1, CA, CB - CA))
                go(one(order[2], j, 8, up2))
                go(one(order[2], j, 9, dn2))

            def arrive_far():
                one(order[3], j, 2, up1, 0, CA).wait_recv()
                one(order[3], j, 3, dn1, CA, CB - CA).wait_recv()
                go(one(order[3], j, 10, up2))
                go(one(order[3], j, 11, dn2))

            def second_step(k):
                one(order[k], jdn, 4 + 2 * k, up2).wait_recv()
                if k in (0, 2):
                    go(one(order[k], jdn, 12 + k, up2))
                one(order[k], jup, 5 + 2 * k, dn2).wait_recv()
                if k in (1, 3):
                    go(one(order[k], jup, 12 + k, dn2))

            def last_step(k):
                one(order[k], jfar, 12 + k, up2 if k in (0, 2) else dn2).wait_recv()

            def done():
                for c in sent:
                    c.wait_send()

            return begin, arrive_dn, arrive_up, arrive_far, second_step, last_step, done

        mine = to.at[rows, cols(y)]
        across = remote(mine, mine, m["s_ag_x"].at[l], 0, **{XH: 1 - xh})
        across.start()
        own = walk(Z, xh, 0)
        oth = walk(Y, 1 - xh, 16)
        own[0]()
        to_xl[l] = remote(xl_out, m["xl_in"].at[l], m["s_xl"].at[l], 0, **{XL: 1 - xl})
        to_xl[l].start()

        @pl.loop(0, SEQ // 32)
        def _(r):
            at = pl.ds(pl.multiple_of(r * 32, 32), 32)
            here = T[at, dp_cols(xl)].astype(F32) + m["core_in"][l, xl, at, :].astype(F32)
            m["dw"][at, :] = here

        own[1]()
        own[2]()
        theirs = to.at[rows_of(z, 1 - xh), cols(y)]
        remote(theirs, theirs, m["s_ag_x"].at[l], 0, **{XH: 1 - xh}).wait_recv()
        oth[0]()
        own[4](0)
        own[3]()
        oth[1]()
        oth[2]()
        own[4](1)
        oth[4](0)
        own[4](2)
        oth[3]()
        oth[4](1)
        if last:
            for c in to_g1:
                c.wait_recv()
            total = pack[...]
            for n in range(7):
                total = total + gain_in[n]
            gain_in[7] = total
            to_g2 = [
                remote(gain_in.at[7], gain_z.at[n], m["s_g2"], n, **t) for n, t in enumerate(zmates)
            ]
            for c in to_g2:
                c.start()
        own[4](3)
        oth[4](2)
        if last:
            for c in to_g2:
                c.wait_recv()
            total = (gain_in[7] + gain_z[0] + gain_z[1] + gain_z[2]) * (1.0 / 4)
            gain_z[3] = total
            to_g3 = [
                remote(gain_z.at[3], gain_y.at[n], m["s_g3"], n, **t) for n, t in enumerate(ymates)
            ]
            for c in to_g3:
                c.start()
        oth[4](3)
        if last:
            finish_weights(0, to_xl[0])
            for c in to_g3:
                c.wait_recv()
            for n in range(-1, 3):
                ref = gain_z.at[3] if n < 0 else gain_y.at[n]
                yy = lax.rem(y + 3 - n, 4)
                for k in range(9):
                    at = pl.ds(pl.multiple_of(yy * CB + k * 128, 128), 128)
                    gain_out[1:2, at] = ref[k : k + 1, :]
                    gain_out[0:1, at] = ref[9 + k : 10 + k, :]
        for k in range(4):
            own[5](k)
            oth[5](k)

        for ring in (ring_a1, ring_b1, ring_a2, ring_b2):
            ring.drain()
        for c in (kv_pair[l], dkv_pair[l], to_x, across, *to_core, *to_stat):
            c.wait_send()
        own[6]()
        oth[6]()
    to_xl[0].wait_send()
    for c in (*to_g1, *to_g2, *to_g3):
        c.wait_send()


def step(lengths, reach, x, g, gain, wq, wk, wv, wo, cosine, sine):
    sem = pltpu.SemaphoreType.DMA
    hbm = pl.BlockSpec(memory_space=pl.ANY)
    vmem = pl.BlockSpec(memory_space=pltpu.VMEM)
    smem = pl.BlockSpec(memory_space=pltpu.SMEM)
    half = HD // 2
    scratch = dict(
        x=VMEM((2, 96, D), BF16),
        normed=VMEM((SEQ, D), BF16),
        g0=VMEM((SEQ, D), BF16),
        g1=VMEM((SEQ, D), BF16),
        S=VMEM((4, 2, RB, D), BF16),
        T=VMEM((SEQ, D), BF16),
        wkv=VMEM((HD, D), BF16),
        wq=VMEM((D, HD), BF16),
        wo=VMEM((HD, D), BF16),
        x_own=VMEM((LAYERS, RB, CB), BF16),
        recip=VMEM((LAYERS, SEQ, HD), F32),
        kv=VMEM((SEQ, HD), F32),
        kv_send=VMEM((LAYERS, SEQ, HD), BF16),
        kv_in=VMEM((LAYERS, SEQ, HD), BF16),
        q=VMEM((SEQ, HD), BF16),
        keep=VMEM((SEQ, HD), BF16),
        send=VMEM((LAYERS, SEQ, HD), BF16),
        dkv_in=VMEM((LAYERS, SEQ, HD), BF16),
        dkv=VMEM((SEQ, HD), BF16),
        dkv_t=VMEM((HD, SEQ), BF16),
        dq=VMEM((SEQ, HD), BF16),
        dq_t=VMEM((HD, SEQ), BF16),
        att_t=VMEM((HD, SEQ), BF16),
        a1=VMEM((8, 2, RB, CB), BF16),
        b1=VMEM((8, RB, 2 * CB), BF16),
        a2=VMEM((8, RB, CB), BF16),
        b2=VMEM((8, RB, CB), BF16),
        ua=VMEM((4, RB, CB), BF16),
        ub=VMEM((RB, D), BF16),
        va=VMEM((2, RB, CB), BF16),
        x_in=VMEM((RB, CB), BF16),
        stat_out=VMEM((LAYERS, RB, HD), F32),
        stat_in=VMEM((LAYERS, 3, RB, HD), F32),
        core_in=VMEM((LAYERS, 2, SEQ, CB), BF16),
        xl_out=VMEM((SEQ, CB), BF16),
        xl_in=VMEM((LAYERS, SEQ, CB), BF16),
        dw=VMEM((SEQ, CB), F32),
        pack=VMEM((24, 128), F32),
        gain_in=VMEM((8, 24, 128), F32),
        gain_z=VMEM((4, 24, 128), F32),
        gain_y=VMEM((3, 24, 128), F32),
        s_local=sem((32,)),
        s_kv=sem((LAYERS, 2, 1)),
        s_dkv=sem((LAYERS, 2, 1)),
        s_a1=sem((LAYERS, 2, 6)),
        s_b1=sem((LAYERS, 2, 6)),
        s_a2=sem((LAYERS, 2, 6)),
        s_b2=sem((LAYERS, 2, 6)),
        s_x=sem((LAYERS, 2, 1)),
        s_stat=sem((LAYERS, 2, 3)),
        s_core=sem((LAYERS, 2, 2)),
        s_xl=sem((LAYERS, 2, 1)),
        s_g1=sem((2, 7)),
        s_g2=sem((2, 3)),
        s_g3=sem((2, 3)),
        s_ag_x=sem((LAYERS, 2, 1)),
        s_ag=sem((LAYERS, 2, 32)),
    )
    return pl.pallas_call(
        step_kernel,
        in_specs=[smem, smem, hbm, hbm, vmem, hbm, hbm, hbm, hbm, vmem, vmem],
        out_specs=[vmem] * 6,
        out_shape=[
            jax.ShapeDtypeStruct((SEQ, D), BF16),
            jax.ShapeDtypeStruct((LAYERS, CB, HD), F32),
            jax.ShapeDtypeStruct((LAYERS, half, CB), F32),
            jax.ShapeDtypeStruct((LAYERS, half, CB), F32),
            jax.ShapeDtypeStruct((LAYERS, HD, CB), F32),
            jax.ShapeDtypeStruct((LAYERS, D), F32),
        ],
        scratch_shapes=[scratch],
        compiler_params=pltpu.CompilerParams(
            collective_id=0, has_side_effects=True, vmem_limit_bytes=VMEM_LIMIT
        ),
        name="step",
    )(lengths, reach, x, g, gain, wq, wk, wv, wo, cosine, sine)


def local(layer_inputs, out_grad, gain, w_query, w_key, w_value, w_out, doc_lengths, window_reach):
    cosine, sine = (jnp.asarray(t) for t in rope_tables())
    wk, wv = jnp.swapaxes(w_key, 1, 2), jnp.swapaxes(w_value, 1, 2)
    outs = step(
        doc_lengths, window_reach, layer_inputs, out_grad, gain, w_query, wk, wv, w_out, cosine, sine
    )
    g, dwq, dwk, dwv, dwo, dgain = write_out(*outs)
    return (g, dwq, jnp.swapaxes(dwk, 1, 2), jnp.swapaxes(dwv, 1, 2), dwo, dgain)


def solution(mesh):
    split = Mesh(mesh.devices.reshape(2, 2, 4, 2, 4), (XL, CORE, Y, XH, Z))
    in_specs = (
        P(None, DP, None),
        P(DP, None),
        P(),
        P(None, None, TP),
        P(None, None, TP),
        P(None, None, TP),
        P(None, TP, None),
        P(DP, None),
        P(),
    )
    out_specs = (
        P(DP, None),
        P(None, DP, TP),
        P(None, DP, TP),
        P(None, DP, TP),
        P(None, TP, DP),
        P(),
    )
    return jax.shard_map(local, mesh=split, in_specs=in_specs, out_specs=out_specs, check_vma=False)
```

```python
import functools
import math

import jax
import jax.numpy as jnp
import numpy as np
from jax import lax
from jax.experimental import pallas as pl
from jax.experimental.pallas import tpu as pltpu
from jax.sharding import Mesh
from jax.sharding import PartitionSpec as P

D = 4608
HEADS = 32
HD = 128
SEQ = 384
LAYERS = 2
CB = D // 4
RB = 48
CA = 640
XL, CORE, Y, XH, Z = ("dp_0", "dp_1", "tp_0", "tp_1", "tp_2")
TP = (Y, XH, Z)
DP = (XL, CORE)
MESH = pl.DeviceIdType.MESH
VMEM = pltpu.VMEM
F32 = jnp.float32
BF16 = jnp.bfloat16
VMEM_LIMIT = 54 * 1024 * 1024

softcap = 50.0
epsilon = 1e-06
score_scale = (D // HEADS) ** (-0.5)


def rope_tables():
    half = HD // 2
    freq = np.exp(-np.arange(half, dtype=np.float64) * (2.0 * math.log(10000.0) / HD))
    angles = np.arange(SEQ, dtype=np.float64)[:, None] * freq[None, :]
    cosine, sine = np.cos(angles), np.sin(angles)
    return (
        np.concatenate([cosine, cosine], axis=1).astype(np.float32),
        np.concatenate([-sine, sine], axis=1).astype(np.float32),
    )


def rotate(v, cosine, sine):
    return v * cosine + pltpu.roll(v, HD // 2, 1) * sine


def unrotate(v, cosine, sine):
    return v * cosine - pltpu.roll(v, HD // 2, 1) * sine


def dot_nn(a, b):
    return lax.dot_general(a, b, (((1,), (0,)), ((), ())), preferred_element_type=F32)


def dot_nt(a, b):
    return lax.dot_general(a, b, (((1,), (1,)), ((), ())), preferred_element_type=F32)


def dot_tn(a, b):
    return lax.dot_general(a, b, (((0,), (0,)), ((), ())), preferred_element_type=F32)


def add(*parts):
    return functools.reduce(lambda a, b: a + b, [p[...].astype(F32) for p in parts])


class Ring:
    def __init__(self, axis, src, buf, sems, out):
        i = lax.axis_index(axis)
        up, dn, far = lax.rem(i + 1, 4), lax.rem(i + 3, 4), lax.rem(i + 2, 4)
        low, high = pl.ds(0, CA), pl.ds(CA, CB - CA)
        self.first = buf.at[0, :, low], buf.at[0, :, high]
        self.turned = buf.at[3, :, low], buf.at[3, :, high]
        self.direct, self.summed = buf.at[1], buf.at[2]
        plan = [
            (src(far, 0), self.first[0], up),
            (src(far, 1), self.first[1], dn),
            (src(up, 1), buf.at[1, :, high], up),
            (src(dn, 0), buf.at[1, :, low], dn),
            (self.turned[0], buf.at[2, :, low], up),
            (self.turned[1], buf.at[2, :, high], dn),
        ]
        self.copies = [
            pltpu.make_async_remote_copy(
                src_ref=s,
                dst_ref=d,
                send_sem=sems.at[0, n],
                recv_sem=sems.at[1, n],
                device_id={axis: to},
                device_id_type=MESH,
            )
            for n, (s, d, to) in enumerate(plan)
        ]
        self.i, self.sides, self.src, self.out = i, (up, dn), src, out

    def start(self, *which):
        for n in which:
            self.copies[n].start()

    def middle(self, *which):
        for h in which:
            self.copies[h].wait_recv()
            self.turned[h][...] = add(self.first[h], self.src(self.sides[h], h)).astype(BF16)
            self.copies[4 + h].start()

    def finish(self):
        for n in range(2, 6):
            self.copies[n].wait_recv()
        self.out[...] = add(self.src(self.i, None), self.direct, self.summed).astype(BF16)

    def drain(self):
        for c in self.copies:
            c.wait_send()


def write_kernel(*refs):
    *refs, sems = refs
    n = len(refs) // 2
    copies = [pltpu.make_async_copy(refs[k], refs[n + k], sems.at[k]) for k in range(n)]
    for c in copies:
        c.start()
    for c in copies:
        c.wait()


def write_out(*arrays):
    arrays = [pltpu.with_memory_space_constraint(a, pltpu.VMEM) for a in arrays]
    return pl.pallas_call(
        write_kernel,
        in_specs=[pl.BlockSpec(memory_space=pltpu.VMEM)] * len(arrays),
        out_specs=[pl.BlockSpec(memory_space=pl.ANY)] * len(arrays),
        out_shape=[jax.ShapeDtypeStruct(a.shape, a.dtype) for a in arrays],
        scratch_shapes=[pltpu.SemaphoreType.DMA((len(arrays),))],
        compiler_params=pltpu.CompilerParams(vmem_limit_bytes=1024 * 1024),
        name="write_out",
    )(*arrays)


def step_kernel(
    lengths,
    reach,
    x_hbm,
    g_hbm,
    gain,
    wq_hbm,
    wk_hbm,
    wv_hbm,
    wo_hbm,
    cosine,
    sine,
    g_out,
    dwq,
    dwk,
    dwv,
    dwo,
    gain_out,
    m,
):
    xl, core, y, xh, z = (lax.axis_index(a) for a in (XL, CORE, Y, XH, Z))
    half = HD // 2

    def remote(src, dst, sems, n, **to):
        return pltpu.make_async_remote_copy(
            src_ref=src,
            dst_ref=dst,
            send_sem=sems.at[0, n],
            recv_sem=sems.at[1, n],
            device_id=to,
            device_id_type=MESH,
        )

    def rows_of(zz, hh):
        return pl.ds(pl.multiple_of(zz * 96 + hh * RB, 16), RB)

    def cols(t, width=CB, shift=0):
        return pl.ds(pl.multiple_of(t * CB + shift, 128), width)

    ymates = [{Y: lax.rem(y + k, 4)} for k in (1, 2, 3)]
    zmates = [{Z: lax.rem(z + k, 4)} for k in (1, 2, 3)]
    xmates = [
        {XL: lax.rem(xl + a, 2), CORE: lax.rem(core + b, 2), XH: lax.rem(xh + c, 2)}
        for a in (0, 1)
        for b in (0, 1)
        for c in (0, 1)
        if a + b + c
    ]
    pair = {Z: z + 1 - 2 * lax.rem(z, 2)}
    even = lax.rem(z, 2) == 0

    def fetch(n, src, dst):
        return pltpu.make_async_copy(src, dst, m["s_local"].at[n])

    get_x, get_wkv, get_wq, get_wo, get_own = {}, {}, {}, {}, {}
    for l in (1, 0):
        get_x[l] = [
            fetch(16 * l + c, x_hbm.at[l, pl.ds(c * 96, 96)], m["x"].at[c % 2])
            for c in range(4)
        ]
        get_wkv[l] = [
            fetch(16 * l + 4, wk_hbm.at[l], m["wkv"].at[pl.ds(0, half)]),
            fetch(16 * l + 5, wv_hbm.at[l], m["wkv"].at[pl.ds(half, half)]),
        ]
        get_wq[l] = fetch(16 * l + 6, wq_hbm.at[l], m["wq"])
        get_wo[l] = fetch(16 * l + 7, wo_hbm.at[l], m["wo"])
        get_own[l] = fetch(16 * l + 8, x_hbm.at[l, rows_of(z, xh), cols(y)], m["x_own"].at[l])
    get_g = fetch(9, g_hbm, m["g0"])
    for c in (*get_x[1][:2], *get_wkv[1], get_wq[1], get_wo[1], get_g, get_own[1]):
        c.start()
    get_own[0].start()

    barrier = pltpu.get_barrier_semaphore()
    for to in (*ymates, *zmates, *xmates):
        pl.semaphore_signal(barrier, inc=1, device_id=to, device_id_type=MESH)

    kv_pair = [remote(m["kv_send"].at[l], m["kv_in"].at[l], m["s_kv"].at[l], 0, **pair) for l in (0, 1)]
    cs, sn = cosine, sine

    def front_norm(l, c):
        x, normed = m["x"], m["normed"]
        get_x[l][c].wait()

        @pl.loop(0, 2)
        def _(r):
            at = pl.ds(pl.multiple_of(c * 96 + r * RB, 16), RB)
            there = pl.ds(pl.multiple_of(r * RB, 16), RB)
            squares = jnp.zeros((RB, HD), F32)
            for k in range(D // HD):
                col = slice(k * HD, (k + 1) * HD)
                v = x[c % 2, there, col].astype(F32)
                squares = squares + v * v
                normed[at, col] = (v * gain[l : l + 1, col]).astype(BF16)
            m["squares"][at, :] = squares

        if c < 2:
            get_x[l][c + 2].start()
        elif l == 1:
            get_x[0][c - 2].start()

    def front_kv(l):
        rc = jnp.sum(m["squares"][...], axis=1, keepdims=True) * (1.0 / D)
        m["recip"][l] = jnp.broadcast_to(lax.rsqrt(rc + epsilon), (SEQ, HD))
        for c in get_wkv[l]:
            c.wait()
        acc = jnp.zeros((SEQ, HD), F32)
        for c in range(3):
            at = slice(c * 1536, (c + 1) * 1536)
            acc = acc + dot_nt(m["normed"][:, at], m["wkv"][:, at])
        acc = acc * m["recip"][l]
        m["kv"][...] = acc
        m["kv_send"][l] = acc.astype(BF16)
        if l == 1:
            pl.semaphore_wait(barrier, 13)
        kv_pair[l].start()

    def front_q(l):
        get_wq[l].wait()
        acc = jnp.zeros((SEQ, HD), F32)
        for c in range(3):
            at = slice(c * 1536, (c + 1) * 1536)
            acc = acc + dot_nn(m["normed"][:, at], m["wq"][at, :])
        m["q"][...] = rotate(acc * m["recip"][l], cs[...], sn[...]).astype(BF16)

    low = lax.broadcasted_iota(jnp.int32, (SEQ, HD), 1) < half

    def attention(l, g):
        if l == 1:
            get_g.wait()
        get_wo[l].wait()
        ga = jnp.zeros((SEQ, HD), F32)
        for c in range(3):
            at = slice(c * 1536, (c + 1) * 1536)
            ga = ga + dot_nt(g[:, at], m["wo"][:, at])
        ga = ga.astype(BF16)

        kv_pair[l].wait_recv()
        own, other = m["kv"][...], m["kv_in"][l].astype(F32)
        first = jnp.where(even, own, other)
        second = jnp.where(even, other, own)
        k_raw = jnp.where(low, first, pltpu.roll(second, half, 1))
        v_raw = jnp.where(low, pltpu.roll(first, half, 1), second)
        k = rotate(k_raw, cs[...], sn[...]).astype(BF16)
        v = v_raw.astype(BF16)

        e0 = lengths[0, 0]
        e1 = e0 + lengths[0, 1]
        e2 = e1 + lengths[0, 2]
        span = reach[l]

        def doc(pos):
            return (
                (pos >= e0).astype(jnp.int32)
                + (pos >= e1).astype(jnp.int32)
                + (pos >= e2).astype(jnp.int32)
            )

        i = lax.broadcasted_iota(jnp.int32, (SEQ, SEQ), 0)
        j = lax.broadcasted_iota(jnp.int32, (SEQ, SEQ), 1)
        doc_i = doc(lax.broadcasted_iota(jnp.int32, (SEQ, 1), 0))
        doc_j = doc(lax.broadcasted_iota(jnp.int32, (1, SEQ), 1))
        allowed = (doc_i == doc_j) & (j <= i) & (i - j < span)

        q = m["q"][...]
        squashed = jnp.tanh(dot_nt(q, k) * (score_scale / softcap))
        raised = jnp.where(allowed, jnp.exp(softcap * squashed), 0.0)
        prob = raised / jnp.sum(raised, axis=1, keepdims=True)
        rounded = prob.astype(BF16)
        att = dot_nn(rounded, v).astype(BF16)
        delta = jnp.sum(ga.astype(F32) * att.astype(F32), axis=1, keepdims=True)
        ds = prob * (dot_nt(ga, v) - delta) * (1.0 - squashed * squashed) * score_scale
        ds = ds.astype(BF16)
        dk_turned = dot_tn(ds, q)
        dv = dot_tn(rounded, ga)
        dk = unrotate(dk_turned, cs[...], sn[...])
        lower = jnp.where(low, dk, pltpu.roll(dv, half, 1))
        upper = jnp.where(low, pltpu.roll(dk, half, 1), dv)
        m["keep"][...] = jnp.where(even, lower, upper).astype(BF16)
        m["send"][l] = jnp.where(even, upper, lower).astype(BF16)
        dkv_pair[l].start()
        dq_turned = dot_nn(ds, k)
        stat = dq_turned * q.astype(F32) + dk_turned * k.astype(F32) + dv * v.astype(F32)
        stat = jnp.sum(stat, axis=1, keepdims=True)
        m["stat_out"][l, 0] = jnp.broadcast_to(stat, (SEQ, HD)).T[:8]
        for c in stat_y[l]:
            c.start()
        dq = unrotate(dq_turned, cs[...], sn[...])
        m["dq"][...] = dq.astype(BF16)
        m["dqkv_t"][:HD] = (dq * m["recip"][l]).astype(BF16).T
        m["att_t"][...] = att.T

    stat_y, stat_z, stat_x = (
        [
            [
                remote(
                    m["stat_out"].at[l, step],
                    m["stat_in"].at[l, 3 * step + n],
                    m["s_stat"].at[l],
                    3 * step + n,
                    **t,
                )
                for n, t in enumerate(mates)
            ]
            for l in (0, 1)
        ]
        for step, mates in enumerate((ymates, zmates, [{XH: 1 - xh}]))
    )

    def stat_sum(l, step, copies):
        for c in copies:
            c.wait_recv()
        total = m["stat_out"][l, step]
        for n in range(len(copies)):
            total = total + m["stat_in"][l, 3 * step + n]
        return total

    dkv_pair = [remote(m["send"].at[l], m["dkv_in"].at[l], m["s_dkv"].at[l], 0, **pair) for l in (0, 1)]

    S, T = m["S"], m["T"]

    def dp_cols(k):
        return pl.ds(pl.multiple_of((2 * k + core) * CB, 128), CB)

    def finish_weights(l, quarter):
        cuts = (0, 3, 5, 7, 9)

        @pl.loop(cuts[quarter], cuts[quarter + 1])
        def _(k):
            at = pl.ds(pl.multiple_of(k * 128, 128), 128)
            v = (m["dw"][:, at] + m["xl_in"][l, :, at].astype(F32)) * (1.0 / 4)
            dwq[l, at, :] = v[:HD].T
            dwk[l, :, at] = v[HD : HD + half]
            dwv[l, :, at] = v[HD + half : 2 * HD]
            dwo[l, :, at] = v[2 * HD :]

    for c in range(4):
        front_norm(1, c)
    front_kv(1)
    front_q(1)
    pack = m["pack"]
    pack[...] = jnp.zeros((24, 128), F32)
    to_xl = {}
    waiting = []
    for l in (1, 0):
        last = l == 0
        g, to = (m["g1"], g_out) if last else (m["g0"], m["g1"])
        attention(l, g)
        if not last:
            get_wo[0].start()
        normed = m["normed"]

        @pl.loop(0, D // 512)
        def _(c):
            at = pl.ds(pl.multiple_of(c * 512, 512), 512)
            T[2 * HD :, at] = dot_nn(m["att_t"][...], g[:, at]).astype(BF16)

        dkv_pair[l].wait_recv()
        dkv = add(m["keep"], m["dkv_in"].at[l])
        m["dkv"][...] = dkv.astype(BF16)
        m["dqkv_t"][HD:] = (dkv * m["recip"][l]).astype(BF16).T
        m["stat_out"][l, 1] = stat_sum(l, 0, stat_y[l])
        for c in stat_z[l]:
            c.start()

        ua, ub, va = m["ua"], m["ub"], m["va"]
        spans = ((0, CA), (CA, CB - CA), (0, CB))
        ring_a, ring_b = {}, {}

        def sub(t, h):
            shift, width = spans[2 if h is None else h]
            return cols(t, width, shift)

        def ring(n, axis, src, out):
            return Ring(axis, src, m["ring"].at[n], m["s_ring"].at[l, n], out)

        for n, k in enumerate((2, 1, 3, 0)):
            zk, yk = lax.rem(z + k, 4), lax.rem(y + k, 4)
            ring_a[k] = ring(n, Y, lambda t, h, zk=zk: S.at[zk, 0, :, sub(t, h)], ua.at[zk])
            ring_b[k] = ring(4 + n, Z, lambda t, h, yk=yk: S.at[t, 1, :, sub(yk, h)], ub.at[yk])
        a2 = ring(8, Z, lambda t, h: ua.at[t, :, pl.ds(*spans[2 if h is None else h])], va.at[0])
        b2 = ring(9, Y, lambda t, h: ub.at[t, :, pl.ds(*spans[2 if h is None else h])], va.at[1])

        for k in (2, 1, 3, 0):

            @pl.loop(0, 3)
            def _(c):
                at = pl.ds(pl.multiple_of(lax.rem(y + k, 4) * CB + c * 384, 128), 384)
                v = dot_nt(m["dq"][...], m["wq"][at, :])
                v = v + dot_nn(m["dkv"][...], m["wkv"][:, at])
                S[:, :, :, at] = v.astype(BF16).reshape(4, 2, RB, 384)

            if k in (2, 1):
                ring_b[k].start(0, 1, 2, 3)
        ring_a[2].start(0, 1, 2, 3)
        ring_a[1].start(0, 1, 2, 3)
        if not last:
            for c in (*get_wkv[0], get_wq[0]):
                c.start()

        @pl.loop(0, D // 512)
        def _(c):
            at = pl.ds(pl.multiple_of(c * 512, 512), 512)
            T[: 2 * HD, at] = dot_nn(m["dqkv_t"][...], normed[:, at]).astype(BF16)

        to_core = [
            remote(
                T.at[:, pl.ds(pl.multiple_of((2 * k + 1 - core) * CB, 128), CB)],
                m["core_in"].at[l, k],
                m["s_core"].at[l],
                k,
                **{CORE: 1 - core},
            )
            for k in (0, 1)
        ]
        to_core[0].start()
        to_core[1].start()

        def aside(c):
            if last:
                finish_weights(1, c)
            else:
                front_norm(0, c)

        def both(do):
            do(ring_b, b2)
            do(ring_a, a2)

        both(lambda r, _: r[2].middle(0, 1))
        both(lambda r, _: r[3].start(0, 1, 2, 3))
        both(lambda r, _: r[1].middle(0, 1))
        both(lambda r, _: r[0].start(0, 1, 2, 3))
        if last:
            to_xl[1].wait_recv()
        aside(0)
        both(lambda r, r2: (r[2].finish(), r2.start(0, 1)))
        m["stat_out"][l, 2] = stat_sum(l, 1, stat_z[l])
        stat_x[l][0].start()
        both(lambda r, _: r[3].middle(0, 1))
        aside(1)
        both(lambda r, r2: (r[1].finish(), r2.start(2)))
        both(lambda r, _: r[0].middle(0, 1))
        aside(2)
        both(lambda r, r2: (r[3].finish(), r2.start(3)))
        both(lambda _, r2: r2.middle(0))
        both(lambda _, r2: r2.middle(1))
        aside(3)
        both(lambda r, r2: (r[0].finish(), r2.finish()))
        to_x = remote(va.at[1 - xh], m["x_in"], m["s_x"].at[l], 0, **{XH: 1 - xh})
        to_x.start()
        if not last:
            front_kv(0)

        total = stat_sum(l, 2, stat_x[l])
        m["stat"][...] = jnp.broadcast_to(total[:1], (HD, SEQ)).T

        for c in to_core:
            c.wait_recv()
        xl_out = m["xl_out"]
        if last:
            to_xl[1].wait_send()

        @pl.loop(0, SEQ // 32)
        def _(r):
            at = pl.ds(pl.multiple_of(r * 32, 32), 32)
            there = T[at, dp_cols(1 - xl)].astype(F32) + m["core_in"][l, 1 - xl, at, :].astype(F32)
            xl_out[at, :] = there.astype(BF16)

        get_own[l].wait()
        to_x.wait_recv()
        rows = rows_of(z, xh)
        grad = add(va.at[xh], m["x_in"])
        rc = m["recip"][l, rows, :][:, :1]
        gn = gain[l : l + 1, cols(y)]
        unit = m["x_own"][l].astype(F32) * rc
        u = grad * gn
        per_feature = jnp.sum(grad * unit, axis=0, keepdims=True)
        for n in range(9):
            k = n + 9 if last else n
            pack[k : k + 1, :] = per_feature[:, n * 128 : (n + 1) * 128]
        if last:
            gain_in, gain_z, gain_y = m["gain_in"], m["gain_z"], m["gain_y"]
            to_g1 = [
                remote(pack, gain_in.at[n], m["s_g1"], n, **t) for n, t in enumerate(xmates)
            ]
            for c in to_g1:
                c.start()
        mean = m["stat"][rows, :][:, :1] * (1.0 / D)
        up_own = g[rows, cols(y)].astype(F32)
        to[rows, cols(y)] = (up_own + rc * (u - unit * mean)).astype(BF16)

        def spread(zz, hh, yy, shift, width, n, dest):
            ref = to.at[rows_of(zz, hh), cols(yy, width, shift)]
            return remote(ref, ref, m["s_ag"].at[l], n, **dest)

        def walk(first_axis, hh, base):
            second = Y if first_axis == Z else Z
            i, j = (z, y) if first_axis == Z else (y, z)
            order = [i, lax.rem(i + 3, 4), lax.rem(i + 1, 4), lax.rem(i + 2, 4)]
            up1, dn1 = {first_axis: lax.rem(i + 1, 4)}, {first_axis: lax.rem(i + 3, 4)}
            up2, dn2 = {second: lax.rem(j + 1, 4)}, {second: lax.rem(j + 3, 4)}
            jdn, jup, jfar = lax.rem(j + 3, 4), lax.rem(j + 1, 4), lax.rem(j + 2, 4)

            def one(ii, jj, n, dest, shift=0, width=CB):
                zz, yy = (ii, jj) if first_axis == Z else (jj, ii)
                return spread(zz, hh, yy, shift, width, base + n, dest)

            sent = []

            def go(c):
                c.start()
                sent.append(c)

            def begin():
                go(one(order[0], j, 0, up1))
                go(one(order[0], j, 1, dn1))
                go(one(order[0], j, 4, up2))
                go(one(order[0], j, 5, dn2))

            def arrive_dn():
                one(order[1], j, 0, up1).wait_recv()
                go(one(order[1], j, 2, up1, 0, CA))

            def arrive_up():
                one(order[2], j, 1, dn1).wait_recv()
                go(one(order[2], j, 3, dn1, CA, CB - CA))

            def arrive_far():
                one(order[3], j, 2, up1, 0, CA).wait_recv()
                one(order[3], j, 3, dn1, CA, CB - CA).wait_recv()

            def across(k):
                go(one(order[k], j, 4 + 2 * k, up2))
                go(one(order[k], j, 5 + 2 * k, dn2))

            def second_step(k):
                one(order[k], jdn, 4 + 2 * k, up2).wait_recv()
                if k in (0, 2):
                    go(one(order[k], jdn, 12 + k, up2))
                one(order[k], jup, 5 + 2 * k, dn2).wait_recv()
                if k in (1, 3):
                    go(one(order[k], jup, 12 + k, dn2))

            def last_step(k):
                one(order[k], jfar, 12 + k, up2 if k in (0, 2) else dn2).wait_recv()

            def done():
                for c in sent:
                    c.wait_send()

            return begin, arrive_dn, arrive_up, arrive_far, second_step, last_step, done, across

        mine = to.at[rows, cols(y)]
        across = remote(mine, mine, m["s_ag_x"].at[l], 0, **{XH: 1 - xh})
        across.start()
        own = walk(Z, xh, 0)
        oth = walk(Y, 1 - xh, 16)
        own[0]()
        to_xl[l] = remote(xl_out, m["xl_in"].at[l], m["s_xl"].at[l], 0, **{XL: 1 - xl})
        to_xl[l].start()

        @pl.loop(0, SEQ // 32)
        def _(r):
            at = pl.ds(pl.multiple_of(r * 32, 32), 32)
            here = T[at, dp_cols(xl)].astype(F32) + m["core_in"][l, xl, at, :].astype(F32)
            m["dw"][at, :] = here

        own[1]()
        own[7](1)
        own[2]()
        theirs = to.at[rows_of(z, 1 - xh), cols(y)]
        remote(theirs, theirs, m["s_ag_x"].at[l], 0, **{XH: 1 - xh}).wait_recv()
        oth[0]()
        own[7](2)
        if not last:
            front_q(0)
        oth[1]()
        oth[7](1)
        oth[2]()
        oth[7](2)
        own[3]()
        own[7](3)
        own[4](0)
        oth[3]()
        oth[7](3)
        own[4](1)
        oth[4](0)
        own[4](2)
        oth[4](1)
        if last:
            for c in to_g1:
                c.wait_recv()
            total = pack[...]
            for n in range(7):
                total = total + gain_in[n]
            gain_in[7] = total
            to_g2 = [
                remote(gain_in.at[7], gain_z.at[n], m["s_g2"], n, **t) for n, t in enumerate(zmates)
            ]
            for c in to_g2:
                c.start()
        own[4](3)
        oth[4](2)
        if last:
            for c in to_g2:
                c.wait_recv()
            total = (gain_in[7] + gain_z[0] + gain_z[1] + gain_z[2]) * (1.0 / 4)
            gain_z[3] = total
            to_g3 = [
                remote(gain_z.at[3], gain_y.at[n], m["s_g3"], n, **t) for n, t in enumerate(ymates)
            ]
            for c in to_g3:
                c.start()
        oth[4](3)
        if last:
            to_xl[0].wait_recv()
            for c in range(4):
                finish_weights(0, c)
            for c in to_g3:
                c.wait_recv()
            for n in range(-1, 3):
                ref = gain_z.at[3] if n < 0 else gain_y.at[n]
                yy = lax.rem(y + 3 - n, 4)
                for k in range(9):
                    at = pl.ds(pl.multiple_of(yy * CB + k * 128, 128), 128)
                    gain_out[1:2, at] = ref[k : k + 1, :]
                    gain_out[0:1, at] = ref[9 + k : 10 + k, :]
        for k in range(4):
            own[5](k)
            oth[5](k)

        for r in (*ring_a.values(), *ring_b.values(), a2, b2):
            r.drain()
        for c in (kv_pair[l], dkv_pair[l], to_x, across, *to_core, *stat_y[l], *stat_z[l], *stat_x[l]):
            c.wait_send()
        own[6]()
        oth[6]()
    to_xl[0].wait_send()
    for c in (*to_g1, *to_g2, *to_g3):
        c.wait_send()


def step(lengths, reach, x, g, gain, wq, wk, wv, wo, cosine, sine):
    sem = pltpu.SemaphoreType.DMA
    hbm = pl.BlockSpec(memory_space=pl.ANY)
    vmem = pl.BlockSpec(memory_space=pltpu.VMEM)
    smem = pl.BlockSpec(memory_space=pltpu.SMEM)
    half = HD // 2
    scratch = dict(
        x=VMEM((2, 96, D), BF16),
        normed=VMEM((SEQ, D), BF16),
        g0=VMEM((SEQ, D), BF16),
        g1=VMEM((SEQ, D), BF16),
        S=VMEM((4, 2, RB, D), BF16),
        T=VMEM((SEQ, D), BF16),
        wkv=VMEM((HD, D), BF16),
        wq=VMEM((D, HD), BF16),
        wo=VMEM((HD, D), BF16),
        x_own=VMEM((LAYERS, RB, CB), BF16),
        recip=VMEM((LAYERS, SEQ, HD), F32),
        kv=VMEM((SEQ, HD), F32),
        kv_send=VMEM((LAYERS, SEQ, HD), BF16),
        kv_in=VMEM((LAYERS, SEQ, HD), BF16),
        q=VMEM((SEQ, HD), BF16),
        keep=VMEM((SEQ, HD), BF16),
        send=VMEM((LAYERS, SEQ, HD), BF16),
        dkv_in=VMEM((LAYERS, SEQ, HD), BF16),
        dkv=VMEM((SEQ, HD), BF16),
        dqkv_t=VMEM((2 * HD, SEQ), BF16),
        dq=VMEM((SEQ, HD), BF16),
        att_t=VMEM((HD, SEQ), BF16),
        ring=VMEM((10, 4, RB, CB), BF16),
        ua=VMEM((4, RB, CB), BF16),
        ub=VMEM((4, RB, CB), BF16),
        va=VMEM((2, RB, CB), BF16),
        x_in=VMEM((RB, CB), BF16),
        squares=VMEM((SEQ, HD), F32),
        stat=VMEM((SEQ, HD), F32),
        stat_out=VMEM((LAYERS, 3, 8, SEQ), F32),
        stat_in=VMEM((LAYERS, 7, 8, SEQ), F32),
        core_in=VMEM((LAYERS, 2, SEQ, CB), BF16),
        xl_out=VMEM((SEQ, CB), BF16),
        xl_in=VMEM((LAYERS, SEQ, CB), BF16),
        dw=VMEM((SEQ, CB), F32),
        pack=VMEM((24, 128), F32),
        gain_in=VMEM((8, 24, 128), F32),
        gain_z=VMEM((4, 24, 128), F32),
        gain_y=VMEM((3, 24, 128), F32),
        s_local=sem((32,)),
        s_kv=sem((LAYERS, 2, 1)),
        s_dkv=sem((LAYERS, 2, 1)),
        s_ring=sem((LAYERS, 10, 2, 6)),
        s_x=sem((LAYERS, 2, 1)),
        s_stat=sem((LAYERS, 2, 7)),
        s_core=sem((LAYERS, 2, 2)),
        s_xl=sem((LAYERS, 2, 1)),
        s_g1=sem((2, 7)),
        s_g2=sem((2, 3)),
        s_g3=sem((2, 3)),
        s_ag_x=sem((LAYERS, 2, 1)),
        s_ag=sem((LAYERS, 2, 32)),
    )
    return pl.pallas_call(
        step_kernel,
        in_specs=[smem, smem, hbm, hbm, vmem, hbm, hbm, hbm, hbm, vmem, vmem],
        out_specs=[vmem] * 6,
        out_shape=[
            VMEM((SEQ, D), BF16),
            VMEM((LAYERS, CB, HD), F32),
            VMEM((LAYERS, half, CB), F32),
            VMEM((LAYERS, half, CB), F32),
            VMEM((LAYERS, HD, CB), F32),
            VMEM((LAYERS, D), F32),
        ],
        scratch_shapes=[scratch],
        compiler_params=pltpu.CompilerParams(
            collective_id=0, has_side_effects=True, vmem_limit_bytes=VMEM_LIMIT
        ),
        name="step",
    )(lengths, reach, x, g, gain, wq, wk, wv, wo, cosine, sine)


def local(layer_inputs, out_grad, gain, w_query, w_key, w_value, w_out, doc_lengths, window_reach):
    cosine, sine = (jnp.asarray(t) for t in rope_tables())
    wk, wv = jnp.swapaxes(w_key, 1, 2), jnp.swapaxes(w_value, 1, 2)
    outs = step(
        doc_lengths, window_reach, layer_inputs, out_grad, gain, w_query, wk, wv, w_out, cosine, sine
    )
    g, dwq, dwk, dwv, dwo, dgain = write_out(*outs)
    return (g, dwq, jnp.swapaxes(dwk, 1, 2), jnp.swapaxes(dwv, 1, 2), dwo, dgain)


def solution(mesh):
    split = Mesh(mesh.devices.reshape(2, 2, 4, 2, 4), (XL, CORE, Y, XH, Z))
    in_specs = (
        P(None, DP, None),
        P(DP, None),
        P(),
        P(None, None, TP),
        P(None, None, TP),
        P(None, None, TP),
        P(None, TP, None),
        P(DP, None),
        P(),
    )
    out_specs = (
        P(DP, None),
        P(None, DP, TP),
        P(None, DP, TP),
        P(None, DP, TP),
        P(None, TP, DP),
        P(),
    )
    return jax.shard_map(local, mesh=split, in_specs=in_specs, out_specs=out_specs, check_vma=False)
```

```python
import functools
import math

import jax
import jax.numpy as jnp
import numpy as np
from jax import lax
from jax.experimental import pallas as pl
from jax.experimental.pallas import tpu as pltpu
from jax.sharding import Mesh
from jax.sharding import PartitionSpec as P

D = 4608
HEADS = 32
HD = 128
SEQ = 384
LAYERS = 2
CB = D // 4
RB = 48
CA = 640
XL, CORE, Y, XH, Z = ("dp_0", "dp_1", "tp_0", "tp_1", "tp_2")
TP = (Y, XH, Z)
DP = (XL, CORE)
MESH = pl.DeviceIdType.MESH
VMEM = pltpu.VMEM
F32 = jnp.float32
BF16 = jnp.bfloat16
VMEM_LIMIT = 54 * 1024 * 1024

softcap = 50.0
epsilon = 1e-06
score_scale = (D // HEADS) ** (-0.5)


def rope_tables():
    half = HD // 2
    freq = np.exp(-np.arange(half, dtype=np.float64) * (2.0 * math.log(10000.0) / HD))
    angles = np.arange(SEQ, dtype=np.float64)[:, None] * freq[None, :]
    cosine, sine = np.cos(angles), np.sin(angles)
    return (
        np.concatenate([cosine, cosine], axis=1).astype(np.float32),
        np.concatenate([-sine, sine], axis=1).astype(np.float32),
    )


def rotate(v, cosine, sine):
    return v * cosine + pltpu.roll(v, HD // 2, 1) * sine


def unrotate(v, cosine, sine):
    return v * cosine - pltpu.roll(v, HD // 2, 1) * sine


def dot_nn(a, b):
    return lax.dot_general(a, b, (((1,), (0,)), ((), ())), preferred_element_type=F32)


def dot_nt(a, b):
    return lax.dot_general(a, b, (((1,), (1,)), ((), ())), preferred_element_type=F32)


def dot_tn(a, b):
    return lax.dot_general(a, b, (((0,), (0,)), ((), ())), preferred_element_type=F32)


def add(*parts):
    return functools.reduce(lambda a, b: a + b, [p[...].astype(F32) for p in parts])


class Ring:
    def __init__(self, axis, src, buf, sems, out):
        i = lax.axis_index(axis)
        up, dn, far = lax.rem(i + 1, 4), lax.rem(i + 3, 4), lax.rem(i + 2, 4)
        low, high = pl.ds(0, CA), pl.ds(CA, CB - CA)
        self.first = buf.at[0, :, low], buf.at[0, :, high]
        self.turned = buf.at[3, :, low], buf.at[3, :, high]
        self.direct, self.summed = buf.at[1], buf.at[2]
        plan = [
            (src(far, 0), self.first[0], up),
            (src(far, 1), self.first[1], dn),
            (src(up, 1), buf.at[1, :, high], up),
            (src(dn, 0), buf.at[1, :, low], dn),
            (self.turned[0], buf.at[2, :, low], up),
            (self.turned[1], buf.at[2, :, high], dn),
        ]
        self.copies = [
            pltpu.make_async_remote_copy(
                src_ref=s,
                dst_ref=d,
                send_sem=sems.at[0, n],
                recv_sem=sems.at[1, n],
                device_id={axis: to},
                device_id_type=MESH,
            )
            for n, (s, d, to) in enumerate(plan)
        ]
        self.i, self.sides, self.src, self.out = i, (up, dn), src, out

    def start(self, *which):
        for n in which:
            self.copies[n].start()

    def middle(self, *which):
        for h in which:
            self.copies[h].wait_recv()
            self.turned[h][...] = add(self.first[h], self.src(self.sides[h], h)).astype(BF16)
            self.copies[4 + h].start()

    def finish(self):
        for n in range(2, 6):
            self.copies[n].wait_recv()
        self.out[...] = add(self.src(self.i, None), self.direct, self.summed).astype(BF16)

    def drain(self):
        for c in self.copies:
            c.wait_send()


class Fetch:
    def __init__(self, src, dst, sem, pieces, second=False):
        size = dst.shape[1 if second else 0] // pieces
        at = [(slice(None),) * second + (pl.ds(k * size, size),) for k in range(pieces)]
        self.parts = [pltpu.make_async_copy(src.at[i], dst.at[i], sem) for i in at]
        self.whole = pltpu.make_async_copy(src, dst, sem)

    def start(self):
        for c in self.parts:
            c.start()

    def wait(self):
        self.whole.wait()


def write_kernel(*refs):
    *refs, sems = refs
    n = len(refs) // 2
    pieces = (12, 4, 2, 2, 4, 1)
    copies = [Fetch(refs[k], refs[n + k], sems.at[k], pieces[k], k and k < 5) for k in range(n)]
    for c in copies:
        c.start()
    for c in copies:
        c.wait()


def write_out(*arrays):
    arrays = [pltpu.with_memory_space_constraint(a, pltpu.VMEM) for a in arrays]
    return pl.pallas_call(
        write_kernel,
        in_specs=[pl.BlockSpec(memory_space=pltpu.VMEM)] * len(arrays),
        out_specs=[pl.BlockSpec(memory_space=pl.ANY)] * len(arrays),
        out_shape=[jax.ShapeDtypeStruct(a.shape, a.dtype) for a in arrays],
        scratch_shapes=[pltpu.SemaphoreType.DMA((len(arrays),))],
        compiler_params=pltpu.CompilerParams(vmem_limit_bytes=1024 * 1024),
        name="write_out",
    )(*arrays)


def step_kernel(
    lengths,
    reach,
    x_hbm,
    g_hbm,
    gain,
    wq_hbm,
    wk_hbm,
    wv_hbm,
    wo_hbm,
    cosine,
    sine,
    g_out,
    dwq,
    dwk,
    dwv,
    dwo,
    gain_out,
    m,
):
    xl, core, y, xh, z = (lax.axis_index(a) for a in (XL, CORE, Y, XH, Z))
    half = HD // 2

    def remote(src, dst, sems, n, **to):
        return pltpu.make_async_remote_copy(
            src_ref=src,
            dst_ref=dst,
            send_sem=sems.at[0, n],
            recv_sem=sems.at[1, n],
            device_id=to,
            device_id_type=MESH,
        )

    def rows_of(zz, hh):
        return pl.ds(pl.multiple_of(zz * 96 + hh * RB, 16), RB)

    def cols(t, width=CB, shift=0):
        return pl.ds(pl.multiple_of(t * CB + shift, 128), width)

    ymates = [{Y: lax.rem(y + k, 4)} for k in (1, 2, 3)]
    zmates = [{Z: lax.rem(z + k, 4)} for k in (1, 2, 3)]
    xmates = [
        {XL: lax.rem(xl + a, 2), CORE: lax.rem(core + b, 2), XH: lax.rem(xh + c, 2)}
        for a in (0, 1)
        for b in (0, 1)
        for c in (0, 1)
        if a + b + c
    ]
    pair = {Z: z + 1 - 2 * lax.rem(z, 2)}
    even = lax.rem(z, 2) == 0

    def fetch(n, src, dst, pieces=1):
        return Fetch(src, dst, m["s_local"].at[n], pieces)

    get_x, get_wkv, get_wq, get_wo, get_own = {}, {}, {}, {}, {}
    for l in (1, 0):
        get_x[l] = [
            fetch(16 * l + c, x_hbm.at[l, pl.ds(c * 96, 96)], m["x"].at[c % 2], 6)
            for c in range(4)
        ]
        get_wkv[l] = [
            fetch(16 * l + 4, wk_hbm.at[l], m["wkv"].at[pl.ds(0, half)], 4),
            fetch(16 * l + 5, wv_hbm.at[l], m["wkv"].at[pl.ds(half, half)], 4),
        ]
        get_wq[l] = fetch(16 * l + 6, wq_hbm.at[l], m["wq"], 8)
        get_wo[l] = fetch(16 * l + 7, wo_hbm.at[l], m["wo"], 8)
        get_own[l] = [
            fetch(16 * l + 10 + n, x_hbm.at[l, rows_of(z, hh), cols(y)], m["x_own"].at[l, n])
            for n, hh in enumerate((xh, 1 - xh))
        ]
    get_g = fetch(9, g_hbm, m["g0"], 12)
    for c in (*get_x[1][:2], *get_wkv[1], get_wq[1], get_wo[1], get_g, *get_own[1], *get_own[0]):
        c.start()

    barrier = pltpu.get_barrier_semaphore()
    for to in (*ymates, *zmates, *xmates):
        pl.semaphore_signal(barrier, inc=1, device_id=to, device_id_type=MESH)

    kv_pair = [remote(m["kv_send"].at[l], m["kv_in"].at[l], m["s_kv"].at[l], 0, **pair) for l in (0, 1)]
    cs, sn = cosine, sine

    def front_norm(l, c):
        x, normed = m["x"], m["normed"]
        get_x[l][c].wait()

        @pl.loop(0, 2)
        def _(r):
            at = pl.ds(pl.multiple_of(c * 96 + r * RB, 16), RB)
            there = pl.ds(pl.multiple_of(r * RB, 16), RB)
            squares = jnp.zeros((RB, HD), F32)
            for k in range(D // HD):
                col = slice(k * HD, (k + 1) * HD)
                v = x[c % 2, there, col].astype(F32)
                squares = squares + v * v
                normed[at, col] = (v * gain[l : l + 1, col]).astype(BF16)
            m["squares"][at, :] = squares

        if c < 2:
            get_x[l][c + 2].start()
        elif l == 1:
            get_x[0][c - 2].start()

    def front_kv(l):
        rc = jnp.sum(m["squares"][...], axis=1, keepdims=True) * (1.0 / D)
        m["recip"][l] = jnp.broadcast_to(lax.rsqrt(rc + epsilon), (SEQ, HD))
        for c in get_wkv[l]:
            c.wait()
        acc = jnp.zeros((SEQ, HD), F32)
        for c in range(3):
            at = slice(c * 1536, (c + 1) * 1536)
            acc = acc + dot_nt(m["normed"][:, at], m["wkv"][:, at])
        acc = acc * m["recip"][l]
        m["kv"][...] = acc
        m["kv_send"][l] = acc.astype(BF16)
        if l == 1:
            pl.semaphore_wait(barrier, 13)
        kv_pair[l].start()

    def front_q(l):
        get_wq[l].wait()
        acc = jnp.zeros((SEQ, HD), F32)
        for c in range(3):
            at = slice(c * 1536, (c + 1) * 1536)
            acc = acc + dot_nn(m["normed"][:, at], m["wq"][at, :])
        m["q"][...] = rotate(acc * m["recip"][l], cs[...], sn[...]).astype(BF16)

    low = lax.broadcasted_iota(jnp.int32, (SEQ, HD), 1) < half

    def attention_upstream(l, g):
        if l == 1:
            get_g.wait()
        get_wo[l].wait()
        ga = jnp.zeros((SEQ, HD), F32)
        for c in range(3):
            at = slice(c * 1536, (c + 1) * 1536)
            ga = ga + dot_nt(g[:, at], m["wo"][:, at])
        m["ga"][...] = ga.astype(BF16)

    def attention_forward(l):
        kv_pair[l].wait_recv()
        own, other = m["kv"][...], m["kv_in"][l].astype(F32)
        first = jnp.where(even, own, other)
        second = jnp.where(even, other, own)
        k_raw = jnp.where(low, first, pltpu.roll(second, half, 1))
        v_raw = jnp.where(low, pltpu.roll(first, half, 1), second)
        k = rotate(k_raw, cs[...], sn[...]).astype(BF16)
        v = v_raw.astype(BF16)

        e0 = lengths[0, 0]
        e1 = e0 + lengths[0, 1]
        e2 = e1 + lengths[0, 2]
        span = reach[l]

        def doc(pos):
            return (
                (pos >= e0).astype(jnp.int32)
                + (pos >= e1).astype(jnp.int32)
                + (pos >= e2).astype(jnp.int32)
            )

        i = lax.broadcasted_iota(jnp.int32, (SEQ, SEQ), 0)
        j = lax.broadcasted_iota(jnp.int32, (SEQ, SEQ), 1)
        doc_i = doc(lax.broadcasted_iota(jnp.int32, (SEQ, 1), 0))
        doc_j = doc(lax.broadcasted_iota(jnp.int32, (1, SEQ), 1))
        allowed = (doc_i == doc_j) & (j <= i) & (i - j < span)

        q = m["q"][...]
        squashed = jnp.tanh(dot_nt(q, k) * (score_scale / softcap))
        raised = jnp.where(allowed, jnp.exp(softcap * squashed), 0.0)
        prob = raised / jnp.sum(raised, axis=1, keepdims=True)
        rounded = prob.astype(BF16)
        att = dot_nn(rounded, v).astype(BF16)
        m["k"][...], m["v"][...], m["att"][...] = k, v, att
        m["rounded"][...] = rounded
        m["factor"][...] = prob * (1.0 - squashed * squashed) * score_scale

    def attention_backward(l):
        k, v, q, att, ga = (m[n][...] for n in ("k", "v", "q", "att", "ga"))
        delta = jnp.sum(ga.astype(F32) * att.astype(F32), axis=1, keepdims=True)
        ds = (m["factor"][...] * (dot_nt(ga, v) - delta)).astype(BF16)
        dk_turned = dot_tn(ds, q)
        dv = dot_tn(m["rounded"][...], ga)
        dk = unrotate(dk_turned, cs[...], sn[...])
        lower = jnp.where(low, dk, pltpu.roll(dv, half, 1))
        upper = jnp.where(low, pltpu.roll(dk, half, 1), dv)
        m["keep"][...] = jnp.where(even, lower, upper).astype(BF16)
        m["send"][l] = jnp.where(even, upper, lower).astype(BF16)
        dkv_pair[l].start()
        dq_turned = dot_nn(ds, k)
        stat = dq_turned * q.astype(F32) + dk_turned * k.astype(F32) + dv * v.astype(F32)
        stat = jnp.sum(stat, axis=1, keepdims=True)
        m["stat_out"][l, 0] = jnp.broadcast_to(stat, (SEQ, HD)).T[:8]
        for c in stat_y[l]:
            c.start()
        dq = unrotate(dq_turned, cs[...], sn[...])
        m["dq"][...] = dq.astype(BF16)
        m["dqkv_t"][:HD] = (dq * m["recip"][l]).astype(BF16).T
        m["att_t"][...] = att.T

    stat_y, stat_z, stat_x = (
        [
            [
                remote(
                    m["stat_out"].at[l, step],
                    m["stat_in"].at[l, 3 * step + n],
                    m["s_stat"].at[l],
                    3 * step + n,
                    **t,
                )
                for n, t in enumerate(mates)
            ]
            for l in (0, 1)
        ]
        for step, mates in enumerate((ymates, zmates, [{XH: 1 - xh}]))
    )

    def stat_sum(l, step, copies):
        for c in copies:
            c.wait_recv()
        total = m["stat_out"][l, step]
        for n in range(len(copies)):
            total = total + m["stat_in"][l, 3 * step + n]
        return total

    dkv_pair = [remote(m["send"].at[l], m["dkv_in"].at[l], m["s_dkv"].at[l], 0, **pair) for l in (0, 1)]

    S, T = m["S"], m["T"]

    def dp_cols(k):
        return pl.ds(pl.multiple_of((2 * k + core) * CB, 128), CB)

    def finish_weights(l, quarter):
        cuts = (0, 3, 5, 7, 9)

        @pl.loop(cuts[quarter], cuts[quarter + 1])
        def _(k):
            at = pl.ds(pl.multiple_of(k * 128, 128), 128)
            v = (m["dw"][:, at] + m["xl_in"][l, :, at].astype(F32)) * (1.0 / 4)
            dwq[l, at, :] = v[:HD].T
            dwk[l, :, at] = v[HD : HD + half]
            dwv[l, :, at] = v[HD + half : 2 * HD]
            dwo[l, :, at] = v[2 * HD :]

    for c in range(4):
        front_norm(1, c)
    front_kv(1)
    front_q(1)
    pack = m["pack"]
    pack[...] = jnp.zeros((24, 128), F32)
    to_xl = {}
    waiting = []
    for l in (1, 0):
        last = l == 0
        g, to = (m["g1"], g_out) if last else (m["g0"], m["g1"])
        attention_upstream(l, g)
        if not last:
            attention_forward(1)
        attention_backward(l)
        if not last:
            get_wo[0].start()
        normed = m["normed"]

        @pl.loop(0, D // 512)
        def _(c):
            at = pl.ds(pl.multiple_of(c * 512, 512), 512)
            T[2 * HD :, at] = dot_nn(m["att_t"][...], g[:, at]).astype(BF16)

        dkv_pair[l].wait_recv()
        dkv = add(m["keep"], m["dkv_in"].at[l])
        m["dkv"][...] = dkv.astype(BF16)
        m["dqkv_t"][HD:] = (dkv * m["recip"][l]).astype(BF16).T
        m["stat_out"][l, 1] = stat_sum(l, 0, stat_y[l])
        for c in stat_z[l]:
            c.start()

        ua, ub, va = m["ua"], m["ub"], m["va"]
        spans = ((0, CA), (CA, CB - CA), (0, CB))
        ring_a, ring_b = {}, {}

        def sub(t, h):
            shift, width = spans[2 if h is None else h]
            return cols(t, width, shift)

        def ring(n, axis, src, out):
            return Ring(axis, src, m["ring"].at[n], m["s_ring"].at[l, n], out)

        for n, k in enumerate((2, 1, 3, 0)):
            zk, yk = lax.rem(z + k, 4), lax.rem(y + k, 4)
            ring_a[k] = ring(n, Y, lambda t, h, zk=zk: S.at[zk, 0, :, sub(t, h)], ua.at[zk])
            ring_b[k] = ring(4 + n, Z, lambda t, h, yk=yk: S.at[t, 1, :, sub(yk, h)], ub.at[yk])
        a2 = ring(8, Z, lambda t, h: ua.at[t, :, pl.ds(*spans[2 if h is None else h])], va.at[0])
        b2 = ring(9, Y, lambda t, h: ub.at[t, :, pl.ds(*spans[2 if h is None else h])], va.at[1])

        for k in (2, 1, 3, 0):

            @pl.loop(0, 3)
            def _(c):
                at = pl.ds(pl.multiple_of(lax.rem(y + k, 4) * CB + c * 384, 128), 384)
                v = dot_nt(m["dq"][...], m["wq"][at, :])
                v = v + dot_nn(m["dkv"][...], m["wkv"][:, at])
                S[:, :, :, at] = v.astype(BF16).reshape(4, 2, RB, 384)

            if k == 2:
                ring_b[2].start(0, 1, 2, 3)
                ring_a[2].start(0, 1)
                ring_a[1].start(0, 1)
            elif k == 1:
                ring_b[1].start(0, 1, 2, 3)
                ring_a[2].start(2)
                ring_a[1].start(2)
            elif k == 3:
                ring_a[2].start(3)
                ring_a[1].start(3)
        if not last:
            for c in (*get_wkv[0], get_wq[0]):
                c.start()

        @pl.loop(0, D // 512)
        def _(c):
            at = pl.ds(pl.multiple_of(c * 512, 512), 512)
            T[: 2 * HD, at] = dot_nn(m["dqkv_t"][...], normed[:, at]).astype(BF16)

        to_core = [
            remote(
                T.at[:, pl.ds(pl.multiple_of((2 * k + 1 - core) * CB, 128), CB)],
                m["core_in"].at[l, k],
                m["s_core"].at[l],
                k,
                **{CORE: 1 - core},
            )
            for k in (0, 1)
        ]
        to_core[0].start()
        to_core[1].start()

        def aside(c):
            if last:
                finish_weights(1, c)
            else:
                front_norm(0, c)

        def both(do):
            do(ring_b, b2)
            do(ring_a, a2)

        both(lambda r, _: r[2].middle(0, 1))
        both(lambda r, _: r[3].start(0, 1, 2, 3))
        both(lambda r, _: r[1].middle(0, 1))
        both(lambda r, _: r[0].start(0, 1, 2, 3))
        if last:
            to_xl[1].wait_recv()
        aside(0)
        both(lambda r, r2: (r[2].finish(), r2.start(0, 1)))
        m["stat_out"][l, 2] = stat_sum(l, 1, stat_z[l])
        stat_x[l][0].start()
        both(lambda r, _: r[3].middle(0, 1))
        aside(1)
        both(lambda r, r2: (r[1].finish(), r2.start(2)))
        both(lambda r, _: r[0].middle(0, 1))
        aside(2)
        both(lambda r, r2: (r[3].finish(), r2.start(3)))
        both(lambda _, r2: r2.middle(0))
        both(lambda _, r2: r2.middle(1))
        aside(3)
        both(lambda r, r2: (r[0].finish(), r2.finish()))
        to_x = [
            remote(va.at[hh], m["x_in"].at[l, n], m["s_x"].at[l], n, **{XH: 1 - xh})
            for n, hh in enumerate((1 - xh, xh))
        ]
        to_x[0].start()
        to_x[1].start()
        if not last:
            front_kv(0)

        total = stat_sum(l, 2, stat_x[l])
        m["stat"][...] = jnp.broadcast_to(total[:1], (HD, SEQ)).T

        for c in to_core:
            c.wait_recv()
        xl_out = m["xl_out"]
        if last:
            to_xl[1].wait_send()

        @pl.loop(0, SEQ // 32)
        def _(r):
            at = pl.ds(pl.multiple_of(r * 32, 32), 32)
            there = T[at, dp_cols(1 - xl)].astype(F32) + m["core_in"][l, 1 - xl, at, :].astype(F32)
            xl_out[at, :] = there.astype(BF16)

        def norm_backward(n, hh):
            get_own[l][n].wait()
            to_x[n].wait_recv()
            rows = rows_of(z, hh)
            grad = add(va.at[hh], m["x_in"].at[l, n])
            rc = m["recip"][l, rows, :][:, :1]
            unit = m["x_own"][l, n].astype(F32) * rc
            u = grad * gain[l : l + 1, cols(y)]
            mean = m["stat"][rows, :][:, :1] * (1.0 / D)
            upper = g[rows, cols(y)].astype(F32)
            to[rows, cols(y)] = (upper + rc * (u - unit * mean)).astype(BF16)
            return jnp.sum(grad * unit, axis=0, keepdims=True)

        per_feature = norm_backward(0, xh)
        def spread(zz, hh, yy, shift, width, n, dest):
            ref = to.at[rows_of(zz, hh), cols(yy, width, shift)]
            return remote(ref, ref, m["s_ag"].at[l], n, **dest)

        def walk(first_axis, hh, base):
            second = Y if first_axis == Z else Z
            i, j = (z, y) if first_axis == Z else (y, z)
            order = [i, lax.rem(i + 3, 4), lax.rem(i + 1, 4), lax.rem(i + 2, 4)]
            up1, dn1 = {first_axis: lax.rem(i + 1, 4)}, {first_axis: lax.rem(i + 3, 4)}
            up2, dn2 = {second: lax.rem(j + 1, 4)}, {second: lax.rem(j + 3, 4)}
            jdn, jup, jfar = lax.rem(j + 3, 4), lax.rem(j + 1, 4), lax.rem(j + 2, 4)

            def one(ii, jj, n, dest, shift=0, width=CB):
                zz, yy = (ii, jj) if first_axis == Z else (jj, ii)
                return spread(zz, hh, yy, shift, width, base + n, dest)

            sent = []

            def go(c):
                c.start()
                sent.append(c)

            def begin():
                go(one(order[0], j, 0, up1))
                go(one(order[0], j, 1, dn1))
                go(one(order[0], j, 4, up2))
                go(one(order[0], j, 5, dn2))

            def arrive_dn():
                one(order[1], j, 0, up1).wait_recv()
                go(one(order[1], j, 2, up1, 0, CA))

            def arrive_up():
                one(order[2], j, 1, dn1).wait_recv()
                go(one(order[2], j, 3, dn1, CA, CB - CA))

            def arrive_far():
                one(order[3], j, 2, up1, 0, CA).wait_recv()
                one(order[3], j, 3, dn1, CA, CB - CA).wait_recv()

            def across(k):
                go(one(order[k], j, 4 + 2 * k, up2))
                go(one(order[k], j, 5 + 2 * k, dn2))

            def second_step(k):
                one(order[k], jdn, 4 + 2 * k, up2).wait_recv()
                if k in (0, 2):
                    go(one(order[k], jdn, 12 + k, up2))
                one(order[k], jup, 5 + 2 * k, dn2).wait_recv()
                if k in (1, 3):
                    go(one(order[k], jup, 12 + k, dn2))

            def last_step(k):
                one(order[k], jfar, 12 + k, up2 if k in (0, 2) else dn2).wait_recv()

            def done():
                for c in sent:
                    c.wait_send()

            return begin, arrive_dn, arrive_up, arrive_far, second_step, last_step, done, across

        own = walk(Z, xh, 0)
        oth = walk(Y, 1 - xh, 16)
        own[0]()
        norm_backward(1, 1 - xh)
        oth[0]()
        for n in range(9):
            k = n + 9 if last else n
            pack[k : k + 1, :] = per_feature[:, n * 128 : (n + 1) * 128]
        if last:
            gain_in, gain_z, gain_y = m["gain_in"], m["gain_z"], m["gain_y"]
            to_g1 = [
                remote(pack, gain_in.at[n], m["s_g1"], n, **t) for n, t in enumerate(xmates)
            ]
            for c in to_g1:
                c.start()
        to_xl[l] = remote(xl_out, m["xl_in"].at[l], m["s_xl"].at[l], 0, **{XL: 1 - xl})
        to_xl[l].start()
        own[1]()
        own[7](1)
        own[2]()

        @pl.loop(0, SEQ // 32)
        def _(r):
            at = pl.ds(pl.multiple_of(r * 32, 32), 32)
            here = T[at, dp_cols(xl)].astype(F32) + m["core_in"][l, xl, at, :].astype(F32)
            m["dw"][at, :] = here

        oth[1]()
        oth[7](1)
        oth[2]()
        own[7](2)
        oth[7](2)
        own[3]()
        own[7](3)
        oth[3]()
        oth[7](3)
        own[4](0)
        if not last:
            front_q(0)
        oth[4](0)
        own[4](1)
        oth[4](1)
        own[4](2)
        if last:
            for c in to_g1:
                c.wait_recv()
            total = pack[...]
            for n in range(7):
                total = total + gain_in[n]
            gain_in[7] = total
            to_g2 = [
                remote(gain_in.at[7], gain_z.at[n], m["s_g2"], n, **t) for n, t in enumerate(zmates)
            ]
            for c in to_g2:
                c.start()
        own[4](3)
        oth[4](2)
        if last:
            for c in to_g2:
                c.wait_recv()
            total = (gain_in[7] + gain_z[0] + gain_z[1] + gain_z[2]) * (1.0 / 4)
            gain_z[3] = total
            to_g3 = [
                remote(gain_z.at[3], gain_y.at[n], m["s_g3"], n, **t) for n, t in enumerate(ymates)
            ]
            for c in to_g3:
                c.start()
        oth[4](3)
        if last:
            to_xl[0].wait_recv()
            for c in range(4):
                finish_weights(0, c)
            for c in to_g3:
                c.wait_recv()
            for n in range(-1, 3):
                ref = gain_z.at[3] if n < 0 else gain_y.at[n]
                yy = lax.rem(y + 3 - n, 4)
                for k in range(9):
                    at = pl.ds(pl.multiple_of(yy * CB + k * 128, 128), 128)
                    gain_out[1:2, at] = ref[k : k + 1, :]
                    gain_out[0:1, at] = ref[9 + k : 10 + k, :]
        if not last:
            attention_forward(0)
        for k in range(4):
            own[5](k)
            oth[5](k)

        for r in (*ring_a.values(), *ring_b.values(), a2, b2):
            r.drain()
        for c in (kv_pair[l], dkv_pair[l], *to_x, *to_core, *stat_y[l], *stat_z[l], *stat_x[l]):
            c.wait_send()
        own[6]()
        oth[6]()
    to_xl[0].wait_send()
    for c in (*to_g1, *to_g2, *to_g3):
        c.wait_send()


def step(lengths, reach, x, g, gain, wq, wk, wv, wo, cosine, sine):
    sem = pltpu.SemaphoreType.DMA
    hbm = pl.BlockSpec(memory_space=pl.ANY)
    vmem = pl.BlockSpec(memory_space=pltpu.VMEM)
    smem = pl.BlockSpec(memory_space=pltpu.SMEM)
    half = HD // 2
    scratch = dict(
        x=VMEM((2, 96, D), BF16),
        normed=VMEM((SEQ, D), BF16),
        g0=VMEM((SEQ, D), BF16),
        g1=VMEM((SEQ, D), BF16),
        S=VMEM((4, 2, RB, D), BF16),
        T=VMEM((SEQ, D), BF16),
        wkv=VMEM((HD, D), BF16),
        wq=VMEM((D, HD), BF16),
        wo=VMEM((HD, D), BF16),
        x_own=VMEM((LAYERS, 2, RB, CB), BF16),
        recip=VMEM((LAYERS, SEQ, HD), F32),
        kv=VMEM((SEQ, HD), F32),
        kv_send=VMEM((LAYERS, SEQ, HD), BF16),
        kv_in=VMEM((LAYERS, SEQ, HD), BF16),
        q=VMEM((SEQ, HD), BF16),
        k=VMEM((SEQ, HD), BF16),
        v=VMEM((SEQ, HD), BF16),
        att=VMEM((SEQ, HD), BF16),
        ga=VMEM((SEQ, HD), BF16),
        rounded=VMEM((SEQ, SEQ), BF16),
        factor=VMEM((SEQ, SEQ), F32),
        keep=VMEM((SEQ, HD), BF16),
        send=VMEM((LAYERS, SEQ, HD), BF16),
        dkv_in=VMEM((LAYERS, SEQ, HD), BF16),
        dkv=VMEM((SEQ, HD), BF16),
        dqkv_t=VMEM((2 * HD, SEQ), BF16),
        dq=VMEM((SEQ, HD), BF16),
        att_t=VMEM((HD, SEQ), BF16),
        ring=VMEM((10, 4, RB, CB), BF16),
        ua=VMEM((4, RB, CB), BF16),
        ub=VMEM((4, RB, CB), BF16),
        va=VMEM((2, RB, CB), BF16),
        x_in=VMEM((LAYERS, 2, RB, CB), BF16),
        squares=VMEM((SEQ, HD), F32),
        stat=VMEM((SEQ, HD), F32),
        stat_out=VMEM((LAYERS, 3, 8, SEQ), F32),
        stat_in=VMEM((LAYERS, 7, 8, SEQ), F32),
        core_in=VMEM((LAYERS, 2, SEQ, CB), BF16),
        xl_out=VMEM((SEQ, CB), BF16),
        xl_in=VMEM((LAYERS, SEQ, CB), BF16),
        dw=VMEM((SEQ, CB), F32),
        pack=VMEM((24, 128), F32),
        gain_in=VMEM((8, 24, 128), F32),
        gain_z=VMEM((4, 24, 128), F32),
        gain_y=VMEM((3, 24, 128), F32),
        s_local=sem((32,)),
        s_kv=sem((LAYERS, 2, 1)),
        s_dkv=sem((LAYERS, 2, 1)),
        s_ring=sem((LAYERS, 10, 2, 6)),
        s_x=sem((LAYERS, 2, 2)),
        s_stat=sem((LAYERS, 2, 7)),
        s_core=sem((LAYERS, 2, 2)),
        s_xl=sem((LAYERS, 2, 1)),
        s_g1=sem((2, 7)),
        s_g2=sem((2, 3)),
        s_g3=sem((2, 3)),
        s_ag=sem((LAYERS, 2, 32)),
    )
    return pl.pallas_call(
        step_kernel,
        in_specs=[smem, smem, hbm, hbm, vmem, hbm, hbm, hbm, hbm, vmem, vmem],
        out_specs=[vmem] * 6,
        out_shape=[
            VMEM((SEQ, D), BF16),
            VMEM((LAYERS, CB, HD), F32),
            VMEM((LAYERS, half, CB), F32),
            VMEM((LAYERS, half, CB), F32),
            VMEM((LAYERS, HD, CB), F32),
            VMEM((LAYERS, D), F32),
        ],
        scratch_shapes=[scratch],
        compiler_params=pltpu.CompilerParams(
            collective_id=0, has_side_effects=True, vmem_limit_bytes=VMEM_LIMIT
        ),
        name="step",
    )(lengths, reach, x, g, gain, wq, wk, wv, wo, cosine, sine)


def local(layer_inputs, out_grad, gain, w_query, w_key, w_value, w_out, doc_lengths, window_reach):
    cosine, sine = (jnp.asarray(t) for t in rope_tables())
    wk, wv = jnp.swapaxes(w_key, 1, 2), jnp.swapaxes(w_value, 1, 2)
    outs = step(
        doc_lengths, window_reach, layer_inputs, out_grad, gain, w_query, wk, wv, w_out, cosine, sine
    )
    g, dwq, dwk, dwv, dwo, dgain = write_out(*outs)
    return (g, dwq, jnp.swapaxes(dwk, 1, 2), jnp.swapaxes(dwv, 1, 2), dwo, dgain)


def solution(mesh):
    split = Mesh(mesh.devices.reshape(2, 2, 4, 2, 4), (XL, CORE, Y, XH, Z))
    in_specs = (
        P(None, DP, None),
        P(DP, None),
        P(),
        P(None, None, TP),
        P(None, None, TP),
        P(None, None, TP),
        P(None, TP, None),
        P(DP, None),
        P(),
    )
    out_specs = (
        P(DP, None),
        P(None, DP, TP),
        P(None, DP, TP),
        P(None, DP, TP),
        P(None, TP, DP),
        P(),
    )
    return jax.shard_map(local, mesh=split, in_specs=in_specs, out_specs=out_specs, check_vma=False)
```

```python
import functools
import math

import jax
import jax.numpy as jnp
import numpy as np
from jax import lax
from jax.experimental import pallas as pl
from jax.experimental.pallas import tpu as pltpu
from jax.sharding import Mesh
from jax.sharding import PartitionSpec as P

D = 4608
HEADS = 32
HD = 128
SEQ = 384
LAYERS = 2
CB = D // 4
RB = 48
CA = 640
XL, CORE, Y, XH, Z = ("dp_0", "dp_1", "tp_0", "tp_1", "tp_2")
TP = (Y, XH, Z)
DP = (XL, CORE)
MESH = pl.DeviceIdType.MESH
VMEM = pltpu.VMEM
F32 = jnp.float32
BF16 = jnp.bfloat16
VMEM_LIMIT = 54 * 1024 * 1024

softcap = 50.0
epsilon = 1e-06
score_scale = (D // HEADS) ** (-0.5)


def rope_tables():
    half = HD // 2
    freq = np.exp(-np.arange(half, dtype=np.float64) * (2.0 * math.log(10000.0) / HD))
    angles = np.arange(SEQ, dtype=np.float64)[:, None] * freq[None, :]
    cosine, sine = np.cos(angles), np.sin(angles)
    return (
        np.concatenate([cosine, cosine], axis=1).astype(np.float32),
        np.concatenate([-sine, sine], axis=1).astype(np.float32),
    )


def rotate(v, cosine, sine):
    return v * cosine + pltpu.roll(v, HD // 2, 1) * sine


def unrotate(v, cosine, sine):
    return v * cosine - pltpu.roll(v, HD // 2, 1) * sine


def dot_nn(a, b):
    return lax.dot_general(a, b, (((1,), (0,)), ((), ())), preferred_element_type=F32)


def dot_nt(a, b):
    return lax.dot_general(a, b, (((1,), (1,)), ((), ())), preferred_element_type=F32)


def dot_tn(a, b):
    return lax.dot_general(a, b, (((0,), (0,)), ((), ())), preferred_element_type=F32)


def add(*parts):
    return functools.reduce(lambda a, b: a + b, [p[...].astype(F32) for p in parts])


class Ring:
    def __init__(self, axis, src, buf, sems, out):
        i = lax.axis_index(axis)
        up, dn, far = lax.rem(i + 1, 4), lax.rem(i + 3, 4), lax.rem(i + 2, 4)
        low, high = pl.ds(0, CA), pl.ds(CA, CB - CA)
        self.first = buf.at[0, :, low], buf.at[0, :, high]
        self.turned = buf.at[3, :, low], buf.at[3, :, high]
        self.direct, self.summed = buf.at[1], buf.at[2]
        plan = [
            (src(far, 0), self.first[0], up),
            (src(far, 1), self.first[1], dn),
            (src(up, 1), buf.at[1, :, high], up),
            (src(dn, 0), buf.at[1, :, low], dn),
            (self.turned[0], buf.at[2, :, low], up),
            (self.turned[1], buf.at[2, :, high], dn),
        ]
        self.copies = [
            pltpu.make_async_remote_copy(
                src_ref=s,
                dst_ref=d,
                send_sem=sems.at[0, n],
                recv_sem=sems.at[1, n],
                device_id={axis: to},
                device_id_type=MESH,
            )
            for n, (s, d, to) in enumerate(plan)
        ]
        self.i, self.sides, self.src, self.out = i, (up, dn), src, out

    def start(self, *which):
        for n in which:
            self.copies[n].start()

    def middle(self, *which):
        for h in which:
            self.copies[h].wait_recv()
            self.turned[h][...] = add(self.first[h], self.src(self.sides[h], h)).astype(BF16)
            self.copies[4 + h].start()

    def finish(self):
        for n in range(2, 6):
            self.copies[n].wait_recv()
        self.out[...] = add(self.src(self.i, None), self.direct, self.summed).astype(BF16)

    def drain(self):
        for c in self.copies:
            c.wait_send()


class Fetch:
    def __init__(self, src, dst, sem, pieces, second=False):
        size = dst.shape[1 if second else 0] // pieces
        at = [(slice(None),) * second + (pl.ds(k * size, size),) for k in range(pieces)]
        self.parts = [pltpu.make_async_copy(src.at[i], dst.at[i], sem) for i in at]
        self.whole = pltpu.make_async_copy(src, dst, sem)

    def start(self):
        for c in self.parts:
            c.start()

    def wait(self):
        self.whole.wait()


def write_kernel(*refs):
    *refs, sems = refs
    n = len(refs) // 2
    pieces = (12, 4, 2, 2, 4, 1)
    copies = [Fetch(refs[k], refs[n + k], sems.at[k], pieces[k], k and k < 5) for k in range(n)]
    for c in copies:
        c.start()
    for c in copies:
        c.wait()


def write_out(*arrays):
    arrays = [pltpu.with_memory_space_constraint(a, pltpu.VMEM) for a in arrays]
    return pl.pallas_call(
        write_kernel,
        in_specs=[pl.BlockSpec(memory_space=pltpu.VMEM)] * len(arrays),
        out_specs=[pl.BlockSpec(memory_space=pl.ANY)] * len(arrays),
        out_shape=[jax.ShapeDtypeStruct(a.shape, a.dtype) for a in arrays],
        scratch_shapes=[pltpu.SemaphoreType.DMA((len(arrays),))],
        compiler_params=pltpu.CompilerParams(vmem_limit_bytes=1024 * 1024),
        name="write_out",
    )(*arrays)


def step_kernel(
    lengths,
    reach,
    x_hbm,
    g_hbm,
    gain,
    wq_hbm,
    wk_hbm,
    wv_hbm,
    wo_hbm,
    cosine,
    sine,
    g_out,
    dwq,
    dwk,
    dwv,
    dwo,
    gain_out,
    m,
):
    xl, core, y, xh, z = (lax.axis_index(a) for a in (XL, CORE, Y, XH, Z))
    half = HD // 2

    def remote(src, dst, sems, n, **to):
        return pltpu.make_async_remote_copy(
            src_ref=src,
            dst_ref=dst,
            send_sem=sems.at[0, n],
            recv_sem=sems.at[1, n],
            device_id=to,
            device_id_type=MESH,
        )

    def rows_of(zz, hh):
        return pl.ds(pl.multiple_of(zz * 96 + hh * RB, 16), RB)

    def cols(t, width=CB, shift=0):
        return pl.ds(pl.multiple_of(t * CB + shift, 128), width)

    ymates = [{Y: lax.rem(y + k, 4)} for k in (1, 2, 3)]
    zmates = [{Z: lax.rem(z + k, 4)} for k in (1, 2, 3)]
    xmates = [
        {XL: lax.rem(xl + a, 2), CORE: lax.rem(core + b, 2), XH: lax.rem(xh + c, 2)}
        for a in (0, 1)
        for b in (0, 1)
        for c in (0, 1)
        if a + b + c
    ]
    pair = {Z: z + 1 - 2 * lax.rem(z, 2)}
    even = lax.rem(z, 2) == 0

    def fetch(n, src, dst, pieces=1):
        return Fetch(src, dst, m["s_local"].at[n], pieces)

    get_x, get_wkv, get_wq, get_wo, get_own = {}, {}, {}, {}, {}
    for l in (1, 0):
        get_x[l] = [
            fetch(16 * l + c, x_hbm.at[l, pl.ds(c * 96, 96)], m["x"].at[c % 2], 6)
            for c in range(4)
        ]
        get_wkv[l] = [
            fetch(16 * l + 4, wk_hbm.at[l], m["wkv"].at[pl.ds(0, half)], 4),
            fetch(16 * l + 5, wv_hbm.at[l], m["wkv"].at[pl.ds(half, half)], 4),
        ]
        get_wq[l] = fetch(16 * l + 6, wq_hbm.at[l], m["wq"], 8)
        get_wo[l] = fetch(16 * l + 7, wo_hbm.at[l], m["wo"], 8)
        get_own[l] = [
            fetch(16 * l + 10 + n, x_hbm.at[l, rows_of(z, hh), cols(y)], m["x_own"].at[l, n])
            for n, hh in enumerate((xh, 1 - xh))
        ]
    get_g = fetch(9, g_hbm, m["g0"], 12)
    for c in (*get_x[1][:2], *get_wkv[1], get_wq[1], get_wo[1], get_g, *get_own[1], *get_own[0]):
        c.start()

    barrier = pltpu.get_barrier_semaphore()
    for to in (*ymates, *zmates, *xmates):
        pl.semaphore_signal(barrier, inc=1, device_id=to, device_id_type=MESH)

    halves = [pl.ds(0, SEQ // 2), pl.ds(SEQ // 2, SEQ // 2)]
    kv_pair = [
        [
            remote(m["kv_send"].at[l, r], m["kv_in"].at[l, r], m["s_kv"].at[l], n, **pair)
            for n, r in enumerate(halves)
        ]
        for l in (0, 1)
    ]
    cs, sn = cosine, sine

    def front_norm(l, c):
        x, normed = m["x"], m["normed"]
        get_x[l][c].wait()

        @pl.loop(0, 2)
        def _(r):
            at = pl.ds(pl.multiple_of(c * 96 + r * RB, 16), RB)
            there = pl.ds(pl.multiple_of(r * RB, 16), RB)
            squares = jnp.zeros((RB, HD), F32)
            for k in range(D // HD):
                col = slice(k * HD, (k + 1) * HD)
                v = x[c % 2, there, col].astype(F32)
                squares = squares + v * v
                normed[at, col] = (v * gain[l : l + 1, col]).astype(BF16)
            m["squares"][at, :] = squares

        if c < 2:
            get_x[l][c + 2].start()
        elif l == 1:
            get_x[0][c - 2].start()

    def front_kv(l, n):
        r = slice(n * SEQ // 2, (n + 1) * SEQ // 2)
        rc = jnp.sum(m["squares"][r, :], axis=1, keepdims=True) * (1.0 / D)
        m["recip"][l, r, :] = jnp.broadcast_to(lax.rsqrt(rc + epsilon), (SEQ // 2, HD))
        if n == 0:
            for c in get_wkv[l]:
                c.wait()
        acc = jnp.zeros((SEQ // 2, HD), F32)
        for c in range(3):
            at = slice(c * 1536, (c + 1) * 1536)
            acc = acc + dot_nt(m["normed"][r, at], m["wkv"][:, at])
        acc = acc * m["recip"][l, r, :]
        m["kv"][r, :] = acc
        m["kv_send"][l, r, :] = acc.astype(BF16)
        if l == 1 and n == 0:
            pl.semaphore_wait(barrier, 13)
        kv_pair[l][n].start()

    def front_q(l):
        get_wq[l].wait()
        acc = jnp.zeros((SEQ, HD), F32)
        for c in range(3):
            at = slice(c * 1536, (c + 1) * 1536)
            acc = acc + dot_nn(m["normed"][:, at], m["wq"][at, :])
        m["q"][...] = rotate(acc * m["recip"][l], cs[...], sn[...]).astype(BF16)

    low = lax.broadcasted_iota(jnp.int32, (SEQ, HD), 1) < half

    def attention_upstream(l, g):
        if l == 1:
            get_g.wait()
        get_wo[l].wait()
        ga = jnp.zeros((SEQ, HD), F32)
        for c in range(3):
            at = slice(c * 1536, (c + 1) * 1536)
            ga = ga + dot_nt(g[:, at], m["wo"][:, at])
        m["ga"][...] = ga.astype(BF16)

    def attention_forward(l):
        for c in kv_pair[l]:
            c.wait_recv()
        own, other = m["kv"][...], m["kv_in"][l].astype(F32)
        first = jnp.where(even, own, other)
        second = jnp.where(even, other, own)
        k_raw = jnp.where(low, first, pltpu.roll(second, half, 1))
        v_raw = jnp.where(low, pltpu.roll(first, half, 1), second)
        k = rotate(k_raw, cs[...], sn[...]).astype(BF16)
        v = v_raw.astype(BF16)

        e0 = lengths[0, 0]
        e1 = e0 + lengths[0, 1]
        e2 = e1 + lengths[0, 2]
        span = reach[l]

        def doc(pos):
            return (
                (pos >= e0).astype(jnp.int32)
                + (pos >= e1).astype(jnp.int32)
                + (pos >= e2).astype(jnp.int32)
            )

        i = lax.broadcasted_iota(jnp.int32, (SEQ, SEQ), 0)
        j = lax.broadcasted_iota(jnp.int32, (SEQ, SEQ), 1)
        doc_i = doc(lax.broadcasted_iota(jnp.int32, (SEQ, 1), 0))
        doc_j = doc(lax.broadcasted_iota(jnp.int32, (1, SEQ), 1))
        allowed = (doc_i == doc_j) & (j <= i) & (i - j < span)

        q = m["q"][...]
        squashed = jnp.tanh(dot_nt(q, k) * (score_scale / softcap))
        raised = jnp.where(allowed, jnp.exp(softcap * squashed), 0.0)
        prob = raised / jnp.sum(raised, axis=1, keepdims=True)
        rounded = prob.astype(BF16)
        att = dot_nn(rounded, v).astype(BF16)
        m["k"][...], m["v"][...], m["att"][...] = k, v, att
        m["rounded"][...] = rounded
        m["factor"][...] = prob * (1.0 - squashed * squashed) * score_scale

    def attention_backward(l):
        k, v, q, att, ga = (m[n][...] for n in ("k", "v", "q", "att", "ga"))
        delta = jnp.sum(ga.astype(F32) * att.astype(F32), axis=1, keepdims=True)
        ds = (m["factor"][...] * (dot_nt(ga, v) - delta)).astype(BF16)
        dk_turned = dot_tn(ds, q)
        dv = dot_tn(m["rounded"][...], ga)
        dk = unrotate(dk_turned, cs[...], sn[...])
        lower = jnp.where(low, dk, pltpu.roll(dv, half, 1))
        upper = jnp.where(low, pltpu.roll(dk, half, 1), dv)
        m["keep"][...] = jnp.where(even, lower, upper).astype(BF16)
        m["send"][l] = jnp.where(even, upper, lower).astype(BF16)
        dkv_pair[l].start()
        dq_turned = dot_nn(ds, k)
        stat = dq_turned * q.astype(F32) + dk_turned * k.astype(F32) + dv * v.astype(F32)
        stat = jnp.sum(stat, axis=1, keepdims=True)
        m["stat_out"][l, 0] = jnp.broadcast_to(stat, (SEQ, HD)).T[:8]
        for c in stat_y[l]:
            c.start()
        dq = unrotate(dq_turned, cs[...], sn[...])
        m["dq"][...] = dq.astype(BF16)
        m["dqkv_t"][:HD] = (dq * m["recip"][l]).astype(BF16).T
        m["att_t"][...] = att.T

    stat_y, stat_z, stat_x = (
        [
            [
                remote(
                    m["stat_out"].at[l, step],
                    m["stat_in"].at[l, 3 * step + n],
                    m["s_stat"].at[l],
                    3 * step + n,
                    **t,
                )
                for n, t in enumerate(mates)
            ]
            for l in (0, 1)
        ]
        for step, mates in enumerate((ymates, zmates, [{XH: 1 - xh}]))
    )

    def stat_sum(l, step, copies):
        for c in copies:
            c.wait_recv()
        total = m["stat_out"][l, step]
        for n in range(len(copies)):
            total = total + m["stat_in"][l, 3 * step + n]
        return total

    dkv_pair = [remote(m["send"].at[l], m["dkv_in"].at[l], m["s_dkv"].at[l], 0, **pair) for l in (0, 1)]

    S, T = m["S"], m["T"]

    def dp_cols(k):
        return pl.ds(pl.multiple_of((2 * k + core) * CB, 128), CB)

    def finish_weights(l, quarter):
        cuts = (0, 3, 5, 7, 9)

        @pl.loop(cuts[quarter], cuts[quarter + 1])
        def _(k):
            at = pl.ds(pl.multiple_of(k * 128, 128), 128)
            v = (m["dw"][:, at] + m["xl_in"][l, :, at].astype(F32)) * (1.0 / 4)
            dwq[l, at, :] = v[:HD].T
            dwk[l, :, at] = v[HD : HD + half]
            dwv[l, :, at] = v[HD + half : 2 * HD]
            dwo[l, :, at] = v[2 * HD :]

    for c in range(4):
        front_norm(1, c)
        if c % 2:
            front_kv(1, c // 2)
    front_q(1)
    pack = m["pack"]
    pack[...] = jnp.zeros((24, 128), F32)
    to_xl = {}
    waiting = []
    for l in (1, 0):
        last = l == 0
        g, to = (m["g1"], g_out) if last else (m["g0"], m["g1"])
        attention_upstream(l, g)
        if not last:
            attention_forward(1)
        attention_backward(l)
        if not last:
            get_wo[0].start()
        normed = m["normed"]

        @pl.loop(0, D // 512)
        def _(c):
            at = pl.ds(pl.multiple_of(c * 512, 512), 512)
            T[2 * HD :, at] = dot_nn(m["att_t"][...], g[:, at]).astype(BF16)

        dkv_pair[l].wait_recv()
        dkv = add(m["keep"], m["dkv_in"].at[l])
        m["dkv"][...] = dkv.astype(BF16)

        ua, ub, va = m["ua"], m["ub"], m["va"]
        spans = ((0, CA), (CA, CB - CA), (0, CB))
        ring_a, ring_b = {}, {}

        def sub(t, h):
            shift, width = spans[2 if h is None else h]
            return cols(t, width, shift)

        def ring(n, axis, src, out):
            return Ring(axis, src, m["ring"].at[n], m["s_ring"].at[l, n], out)

        for n, k in enumerate((2, 1, 3, 0)):
            zk, yk = lax.rem(z + k, 4), lax.rem(y + k, 4)
            ring_a[k] = ring(n, Y, lambda t, h, zk=zk: S.at[zk, 0, :, sub(t, h)], ua.at[zk])
            ring_b[k] = ring(4 + n, Z, lambda t, h, yk=yk: S.at[t, 1, :, sub(yk, h)], ub.at[yk])
        a2 = ring(8, Z, lambda t, h: ua.at[t, :, pl.ds(*spans[2 if h is None else h])], va.at[0])
        b2 = ring(9, Y, lambda t, h: ub.at[t, :, pl.ds(*spans[2 if h is None else h])], va.at[1])

        for k in (2, 1, 3, 0):

            @pl.loop(0, 3)
            def _(c):
                at = pl.ds(pl.multiple_of(lax.rem(y + k, 4) * CB + c * 384, 128), 384)
                v = dot_nt(m["dq"][...], m["wq"][at, :])
                v = v + dot_nn(m["dkv"][...], m["wkv"][:, at])
                S[:, :, :, at] = v.astype(BF16).reshape(4, 2, RB, 384)

            if k == 2:
                ring_b[2].start(0, 1, 2, 3)
                ring_a[2].start(0, 1)
                ring_a[1].start(0, 1)
            elif k == 1:
                ring_b[1].start(0, 1, 2, 3)
                ring_a[2].start(2)
                ring_a[1].start(2)
            elif k == 3:
                ring_a[2].start(3)
                ring_a[1].start(3)
        if not last:
            for c in (*get_wkv[0], get_wq[0]):
                c.start()

        dkv = add(m["keep"], m["dkv_in"].at[l])
        m["dqkv_t"][HD:] = (dkv * m["recip"][l]).astype(BF16).T
        m["stat_out"][l, 1] = stat_sum(l, 0, stat_y[l])
        for c in stat_z[l]:
            c.start()

        @pl.loop(0, D // 512)
        def _(c):
            at = pl.ds(pl.multiple_of(c * 512, 512), 512)
            T[: 2 * HD, at] = dot_nn(m["dqkv_t"][...], normed[:, at]).astype(BF16)

        to_core = [
            remote(
                T.at[:, pl.ds(pl.multiple_of((2 * k + 1 - core) * CB, 128), CB)],
                m["core_in"].at[l, k],
                m["s_core"].at[l],
                k,
                **{CORE: 1 - core},
            )
            for k in (0, 1)
        ]
        to_core[0].start()
        to_core[1].start()

        def aside(c):
            if last:
                finish_weights(1, c)
            else:
                front_norm(0, c)

        def both(do):
            do(ring_b, b2)
            do(ring_a, a2)

        both(lambda r, _: r[2].middle(0, 1))
        both(lambda r, _: r[3].start(0, 1, 2, 3))
        both(lambda r, _: r[1].middle(0, 1))
        both(lambda r, _: r[0].start(0, 1, 2, 3))
        if last:
            to_xl[1].wait_recv()
        aside(0)
        both(lambda r, r2: (r[2].finish(), r2.start(0, 1)))
        both(lambda r, _: r[3].middle(0, 1))
        aside(1)
        both(lambda r, r2: (r[1].finish(), r2.start(2)))
        both(lambda r, _: r[0].middle(0, 1))
        aside(2)
        m["stat_out"][l, 2] = stat_sum(l, 1, stat_z[l])
        stat_x[l][0].start()
        both(lambda r, r2: (r[3].finish(), r2.start(3)))
        both(lambda _, r2: r2.middle(0))
        both(lambda _, r2: r2.middle(1))
        aside(3)
        both(lambda r, r2: (r[0].finish(), r2.finish()))
        to_x = [
            remote(va.at[hh], m["x_in"].at[l, n], m["s_x"].at[l], n, **{XH: 1 - xh})
            for n, hh in enumerate((1 - xh, xh))
        ]
        to_x[0].start()
        to_x[1].start()
        if not last:
            front_kv(0, 0)
            front_kv(0, 1)

        total = stat_sum(l, 2, stat_x[l])
        m["stat"][...] = jnp.broadcast_to(total[:1], (HD, SEQ)).T

        for c in to_core:
            c.wait_recv()
        xl_out = m["xl_out"]
        if last:
            to_xl[1].wait_send()

        @pl.loop(0, SEQ // 32)
        def _(r):
            at = pl.ds(pl.multiple_of(r * 32, 32), 32)
            there = T[at, dp_cols(1 - xl)].astype(F32) + m["core_in"][l, 1 - xl, at, :].astype(F32)
            xl_out[at, :] = there.astype(BF16)

        def norm_backward(n, hh):
            get_own[l][n].wait()
            to_x[n].wait_recv()
            rows = rows_of(z, hh)
            grad = add(va.at[hh], m["x_in"].at[l, n])
            rc = m["recip"][l, rows, :][:, :1]
            unit = m["x_own"][l, n].astype(F32) * rc
            u = grad * gain[l : l + 1, cols(y)]
            mean = m["stat"][rows, :][:, :1] * (1.0 / D)
            upper = g[rows, cols(y)].astype(F32)
            to[rows, cols(y)] = (upper + rc * (u - unit * mean)).astype(BF16)
            return jnp.sum(grad * unit, axis=0, keepdims=True)

        per_feature = norm_backward(0, xh)
        def spread(zz, hh, yy, shift, width, n, dest):
            ref = to.at[rows_of(zz, hh), cols(yy, width, shift)]
            return remote(ref, ref, m["s_ag"].at[l], n, **dest)

        def walk(first_axis, hh, base):
            second = Y if first_axis == Z else Z
            i, j = (z, y) if first_axis == Z else (y, z)
            order = [i, lax.rem(i + 3, 4), lax.rem(i + 1, 4), lax.rem(i + 2, 4)]
            up1, dn1 = {first_axis: lax.rem(i + 1, 4)}, {first_axis: lax.rem(i + 3, 4)}
            up2, dn2 = {second: lax.rem(j + 1, 4)}, {second: lax.rem(j + 3, 4)}
            jdn, jup, jfar = lax.rem(j + 3, 4), lax.rem(j + 1, 4), lax.rem(j + 2, 4)

            def one(ii, jj, n, dest, shift=0, width=CB):
                zz, yy = (ii, jj) if first_axis == Z else (jj, ii)
                return spread(zz, hh, yy, shift, width, base + n, dest)

            sent = []

            def go(c):
                c.start()
                sent.append(c)

            def begin():
                go(one(order[0], j, 0, up1))
                go(one(order[0], j, 1, dn1))
                go(one(order[0], j, 4, up2))
                go(one(order[0], j, 5, dn2))

            def arrive_dn():
                one(order[1], j, 0, up1).wait_recv()
                go(one(order[1], j, 2, up1, 0, CA))

            def arrive_up():
                one(order[2], j, 1, dn1).wait_recv()
                go(one(order[2], j, 3, dn1, CA, CB - CA))

            def arrive_far():
                one(order[3], j, 2, up1, 0, CA).wait_recv()
                one(order[3], j, 3, dn1, CA, CB - CA).wait_recv()

            def across(k):
                go(one(order[k], j, 4 + 2 * k, up2))
                go(one(order[k], j, 5 + 2 * k, dn2))

            def second_step(k):
                one(order[k], jdn, 4 + 2 * k, up2).wait_recv()
                if k in (0, 2):
                    go(one(order[k], jdn, 12 + k, up2))
                one(order[k], jup, 5 + 2 * k, dn2).wait_recv()
                if k in (1, 3):
                    go(one(order[k], jup, 12 + k, dn2))

            def last_step(k):
                one(order[k], jfar, 12 + k, up2 if k in (0, 2) else dn2).wait_recv()

            def done():
                for c in sent:
                    c.wait_send()

            return begin, arrive_dn, arrive_up, arrive_far, second_step, last_step, done, across

        own = walk(Z, xh, 0)
        oth = walk(Y, 1 - xh, 16)
        own[0]()
        norm_backward(1, 1 - xh)
        oth[0]()
        for n in range(9):
            k = n + 9 if last else n
            pack[k : k + 1, :] = per_feature[:, n * 128 : (n + 1) * 128]
        if last:
            gain_in, gain_z, gain_y = m["gain_in"], m["gain_z"], m["gain_y"]
            to_g1 = [
                remote(pack, gain_in.at[n], m["s_g1"], n, **t) for n, t in enumerate(xmates)
            ]
            for c in to_g1:
                c.start()
        to_xl[l] = remote(xl_out, m["xl_in"].at[l], m["s_xl"].at[l], 0, **{XL: 1 - xl})
        to_xl[l].start()
        own[1]()
        own[7](1)
        own[2]()

        @pl.loop(0, SEQ // 32)
        def _(r):
            at = pl.ds(pl.multiple_of(r * 32, 32), 32)
            here = T[at, dp_cols(xl)].astype(F32) + m["core_in"][l, xl, at, :].astype(F32)
            m["dw"][at, :] = here

        oth[1]()
        oth[7](1)
        oth[2]()
        own[7](2)
        oth[7](2)
        own[3]()
        own[7](3)
        oth[3]()
        oth[7](3)
        own[4](0)
        if not last:
            front_q(0)
        oth[4](0)
        own[4](1)
        oth[4](1)
        own[4](2)
        if last:
            for c in to_g1:
                c.wait_recv()
            total = pack[...]
            for n in range(7):
                total = total + gain_in[n]
            gain_in[7] = total
            to_g2 = [
                remote(gain_in.at[7], gain_z.at[n], m["s_g2"], n, **t) for n, t in enumerate(zmates)
            ]
            for c in to_g2:
                c.start()
        own[4](3)
        oth[4](2)
        if last:
            for c in to_g2:
                c.wait_recv()
            total = (gain_in[7] + gain_z[0] + gain_z[1] + gain_z[2]) * (1.0 / 4)
            gain_z[3] = total
            to_g3 = [
                remote(gain_z.at[3], gain_y.at[n], m["s_g3"], n, **t) for n, t in enumerate(ymates)
            ]
            for c in to_g3:
                c.start()
        oth[4](3)
        if last:
            to_xl[0].wait_recv()
            for c in range(4):
                finish_weights(0, c)
            for c in to_g3:
                c.wait_recv()
            for n in range(-1, 3):
                ref = gain_z.at[3] if n < 0 else gain_y.at[n]
                yy = lax.rem(y + 3 - n, 4)
                for k in range(9):
                    at = pl.ds(pl.multiple_of(yy * CB + k * 128, 128), 128)
                    gain_out[1:2, at] = ref[k : k + 1, :]
                    gain_out[0:1, at] = ref[9 + k : 10 + k, :]
        if not last:
            attention_forward(0)
        for k in range(4):
            own[5](k)
            oth[5](k)

        for r in (*ring_a.values(), *ring_b.values(), a2, b2):
            r.drain()
        for c in (*kv_pair[l], dkv_pair[l], *to_x, *to_core, *stat_y[l], *stat_z[l], *stat_x[l]):
            c.wait_send()
        own[6]()
        oth[6]()
    to_xl[0].wait_send()
    for c in (*to_g1, *to_g2, *to_g3):
        c.wait_send()


def step(lengths, reach, x, g, gain, wq, wk, wv, wo, cosine, sine):
    sem = pltpu.SemaphoreType.DMA
    hbm = pl.BlockSpec(memory_space=pl.ANY)
    vmem = pl.BlockSpec(memory_space=pltpu.VMEM)
    smem = pl.BlockSpec(memory_space=pltpu.SMEM)
    half = HD // 2
    scratch = dict(
        x=VMEM((2, 96, D), BF16),
        normed=VMEM((SEQ, D), BF16),
        g0=VMEM((SEQ, D), BF16),
        g1=VMEM((SEQ, D), BF16),
        S=VMEM((4, 2, RB, D), BF16),
        T=VMEM((SEQ, D), BF16),
        wkv=VMEM((HD, D), BF16),
        wq=VMEM((D, HD), BF16),
        wo=VMEM((HD, D), BF16),
        x_own=VMEM((LAYERS, 2, RB, CB), BF16),
        recip=VMEM((LAYERS, SEQ, HD), F32),
        kv=VMEM((SEQ, HD), F32),
        kv_send=VMEM((LAYERS, SEQ, HD), BF16),
        kv_in=VMEM((LAYERS, SEQ, HD), BF16),
        q=VMEM((SEQ, HD), BF16),
        k=VMEM((SEQ, HD), BF16),
        v=VMEM((SEQ, HD), BF16),
        att=VMEM((SEQ, HD), BF16),
        ga=VMEM((SEQ, HD), BF16),
        rounded=VMEM((SEQ, SEQ), BF16),
        factor=VMEM((SEQ, SEQ), F32),
        keep=VMEM((SEQ, HD), BF16),
        send=VMEM((LAYERS, SEQ, HD), BF16),
        dkv_in=VMEM((LAYERS, SEQ, HD), BF16),
        dkv=VMEM((SEQ, HD), BF16),
        dqkv_t=VMEM((2 * HD, SEQ), BF16),
        dq=VMEM((SEQ, HD), BF16),
        att_t=VMEM((HD, SEQ), BF16),
        ring=VMEM((10, 4, RB, CB), BF16),
        ua=VMEM((4, RB, CB), BF16),
        ub=VMEM((4, RB, CB), BF16),
        va=VMEM((2, RB, CB), BF16),
        x_in=VMEM((LAYERS, 2, RB, CB), BF16),
        squares=VMEM((SEQ, HD), F32),
        stat=VMEM((SEQ, HD), F32),
        stat_out=VMEM((LAYERS, 3, 8, SEQ), F32),
        stat_in=VMEM((LAYERS, 7, 8, SEQ), F32),
        core_in=VMEM((LAYERS, 2, SEQ, CB), BF16),
        xl_out=VMEM((SEQ, CB), BF16),
        xl_in=VMEM((LAYERS, SEQ, CB), BF16),
        dw=VMEM((SEQ, CB), F32),
        pack=VMEM((24, 128), F32),
        gain_in=VMEM((8, 24, 128), F32),
        gain_z=VMEM((4, 24, 128), F32),
        gain_y=VMEM((3, 24, 128), F32),
        s_local=sem((32,)),
        s_kv=sem((LAYERS, 2, 2)),
        s_dkv=sem((LAYERS, 2, 1)),
        s_ring=sem((LAYERS, 10, 2, 6)),
        s_x=sem((LAYERS, 2, 2)),
        s_stat=sem((LAYERS, 2, 7)),
        s_core=sem((LAYERS, 2, 2)),
        s_xl=sem((LAYERS, 2, 1)),
        s_g1=sem((2, 7)),
        s_g2=sem((2, 3)),
        s_g3=sem((2, 3)),
        s_ag=sem((LAYERS, 2, 32)),
    )
    return pl.pallas_call(
        step_kernel,
        in_specs=[smem, smem, hbm, hbm, vmem, hbm, hbm, hbm, hbm, vmem, vmem],
        out_specs=[vmem] * 6,
        out_shape=[
            VMEM((SEQ, D), BF16),
            VMEM((LAYERS, CB, HD), F32),
            VMEM((LAYERS, half, CB), F32),
            VMEM((LAYERS, half, CB), F32),
            VMEM((LAYERS, HD, CB), F32),
            VMEM((LAYERS, D), F32),
        ],
        scratch_shapes=[scratch],
        compiler_params=pltpu.CompilerParams(
            collective_id=0, has_side_effects=True, vmem_limit_bytes=VMEM_LIMIT
        ),
        name="step",
    )(lengths, reach, x, g, gain, wq, wk, wv, wo, cosine, sine)


def local(layer_inputs, out_grad, gain, w_query, w_key, w_value, w_out, doc_lengths, window_reach):
    cosine, sine = (jnp.asarray(t) for t in rope_tables())
    wk, wv = jnp.swapaxes(w_key, 1, 2), jnp.swapaxes(w_value, 1, 2)
    outs = step(
        doc_lengths, window_reach, layer_inputs, out_grad, gain, w_query, wk, wv, w_out, cosine, sine
    )
    g, dwq, dwk, dwv, dwo, dgain = write_out(*outs)
    return (g, dwq, jnp.swapaxes(dwk, 1, 2), jnp.swapaxes(dwv, 1, 2), dwo, dgain)


def solution(mesh):
    split = Mesh(mesh.devices.reshape(2, 2, 4, 2, 4), (XL, CORE, Y, XH, Z))
    in_specs = (
        P(None, DP, None),
        P(DP, None),
        P(),
        P(None, None, TP),
        P(None, None, TP),
        P(None, None, TP),
        P(None, TP, None),
        P(DP, None),
        P(),
    )
    out_specs = (
        P(DP, None),
        P(None, DP, TP),
        P(None, DP, TP),
        P(None, DP, TP),
        P(None, TP, DP),
        P(),
    )
    return jax.shard_map(local, mesh=split, in_specs=in_specs, out_specs=out_specs, check_vma=False)
```
